32 devices in a mesh: dp: 4 (over x, y), sp: 8 (over z, core).
Axes of the slice: x: 2, y: 2, z: 4, core: 2. Of those that a mesh axis runs over, the one named last changes fastest.
Arguments:
- x: bfloat16 [4, 16384, 128], P('dp', 'sp'), parts along dimension 0
- w_in: bfloat16 [14, 3, 128, 256], replicated
- w_res: bfloat16 [14, 128, 128], replicated
- w_skip: bfloat16 [14, 128, 128], replicated
Outputs:
- output 1: float32 [4, 16384, 128], P('dp', 'sp'), parts along dimension 0
- output 2: float32 [4, 16384, 128], P('dp', 'sp'), parts along dimension 0
There are 4 independent parts. The reference program is written for one: setup_inputs(seed, part) draws one part's arguments, and reference() takes and returns one part's arrays. A program takes and returns all parts, laid end to end along the dimension named above; an argument that names none is the same for every part.
All inputs are finite; a program needn't handle non-finite values.
Results may differ from the reference program's by a relative error of at most 0.00526473.
Values are sent between devices in bfloat16 or wider.
A program may use at most 1 GiB of HBM per device.

```python
import jax
import jax.numpy as jnp

NUM_SEQS = 1
SEQ_LEN = 16384
CHANNELS = 128
SKIP_CH = 128
NUM_LAYERS = 14


def setup_inputs(seed: int = 0, part: int = 0) -> dict:
    root_key = jax.random.key(seed)
    key_x, key_in, key_res, key_skip = jax.random.split(root_key, 4)
    x = jax.random.normal(jax.random.fold_in(key_x, part), (NUM_SEQS, SEQ_LEN, CHANNELS), jnp.float32)
    w_in = jax.random.normal(key_in, (NUM_LAYERS, 3, CHANNELS, 2 * CHANNELS), jnp.float32) * (3 * CHANNELS) ** -0.5
    w_res = jax.random.normal(key_res, (NUM_LAYERS, CHANNELS, CHANNELS), jnp.float32) * (0.5 * CHANNELS ** -0.5)
    w_skip = jax.random.normal(key_skip, (NUM_LAYERS, CHANNELS, SKIP_CH), jnp.float32) * CHANNELS ** -0.5
    return {'x': x.astype(jnp.bfloat16), 'w_in': w_in.astype(jnp.bfloat16), 'w_res': w_res.astype(jnp.bfloat16), 'w_skip': w_skip.astype(jnp.bfloat16)}


def matmul_rows(operand, weight):
    flat = jnp.dot(operand.reshape(-1, operand.shape[-1]), weight, preferred_element_type=jnp.float32)
    return flat.reshape(operand.shape[:-1] + (weight.shape[-1],))


def reference(x, w_in, w_res, w_skip):
    seq_len = x.shape[1]
    n_chan = x.shape[2]
    residual = x.astype(jnp.float32)
    skip_sum = jnp.zeros(x.shape[:2] + (w_skip.shape[2],), jnp.float32)
    for layer in range(NUM_LAYERS):
        dilation = 2 ** layer
        cur_bf = residual.astype(jnp.bfloat16)
        left_tap = jnp.pad(cur_bf[:, :seq_len - dilation], ((0, 0), (dilation, 0), (0, 0)))
        right_tap = jnp.pad(cur_bf[:, dilation:], ((0, 0), (0, dilation), (0, 0)))
        pre_act = matmul_rows(left_tap, w_in[layer, 0]) + matmul_rows(cur_bf, w_in[layer, 1]) + matmul_rows(right_tap, w_in[layer, 2])
        gated = (jnp.tanh(pre_act[..., :n_chan]) * jax.nn.sigmoid(pre_act[..., n_chan:])).astype(jnp.bfloat16)
        residual = residual + matmul_rows(gated, w_res[layer])
        skip_sum = skip_sum + matmul_rows(gated, w_skip[layer])
    return residual, skip_sum
```

```python
import functools

import jax
import jax.numpy as jnp
from jax import lax
from jax.experimental import pallas as pl
from jax.experimental.pallas import tpu as pltpu
from jax.sharding import PartitionSpec as P

MESH = pl.DeviceIdType.MESH
N_DEV = 8
ROWS = 2048
CH = 128
EXT = 256
PAD = EXT + 16
REACH = [256, 256, 256, 240, 224, 192, 128, 0]
CHUNK = 256
ORDER = [0, 1, 6, 7, 3, 4, 2, 5]


def kernel(x_ref, win_ref, wres_ref, wskip_ref, h_ref, s_ref,
           xb, ha, hb, sk, u4, u5, u6, u7, u8, u9, u10, u11, u12, u13,
           v11l, v11r, v12l, v12r, v13, win, wrs, lsem, wsem, osem, ssem, rsem):
    me = lax.axis_index('sp')
    has_l, has_r = me >= 1, me <= N_DEV - 2
    has_l2, has_r2 = me >= 2, me <= N_DEV - 3
    low = me < N_DEV // 2
    partner = jnp.where(low, me + N_DEV // 2, me - N_DEV // 2)
    have = {-1: has_l, 1: has_r, -2: has_l2, 2: has_r2}

    loads = []
    own_x = pltpu.make_async_copy(x_ref.at[0], xb.at[pl.ds(EXT, ROWS)], lsem)
    own_x.start()
    for k in range(14):
        trio = [pltpu.make_async_copy(win_ref.at[k], win.at[k], wsem.at[k, 0]),
                pltpu.make_async_copy(wres_ref.at[k], wrs.at[k, :, pl.ds(0, CH)], wsem.at[k, 1]),
                pltpu.make_async_copy(wskip_ref.at[k], wrs.at[k, :, pl.ds(CH, CH)], wsem.at[k, 2])]
        for c in trio:
            c.start()
        loads.append(trio)

    barrier = pltpu.get_barrier_semaphore()
    for dj, ok in have.items():
        @pl.when(ok)
        def _():
            pl.semaphore_signal(barrier, inc=1, device_id={'sp': me + dj}, device_id_type=MESH)
    pl.semaphore_signal(barrier, inc=1, device_id={'sp': partner}, device_id_type=MESH)

    def zero(ref, start, count):
        ref[pl.ds(start, count), :] = jnp.zeros((count, CH), ref.dtype)

    @pl.when(jnp.logical_not(has_l))
    def _():
        zero(xb, 0, EXT)
        zero(u8, 0, 256)
        zero(u9, 0, 512)
        zero(u10, 0, 1024)

    @pl.when(jnp.logical_not(has_r))
    def _():
        zero(xb, EXT + ROWS, EXT)
        zero(u8, 256 + ROWS, 256)
        zero(u9, 512 + ROWS, 512)
        zero(u10, 1024 + ROWS, 1024)
    for buf in (ha, hb):
        zero(buf, 0, 16)
        zero(buf, PAD + ROWS + EXT, 16)

    peers = 1
    for ok in have.values():
        peers += jnp.where(ok, 1, 0)
    pl.semaphore_wait(barrier, peers)

    count = [0]
    sent = []

    def remote(src, dst, dj):
        i = count[0]
        count[0] += 1
        dev = partner if dj is None else me + dj
        cp = pltpu.make_async_remote_copy(src_ref=src, dst_ref=dst, send_sem=ssem.at[i], recv_sem=rsem.at[i],
                                          device_id={'sp': dev}, device_id_type=MESH)
        if dj is None:
            cp.start()
        else:
            @pl.when(have[dj])
            def _():
                cp.start()
        sent.append((cp, dj))
        return cp, dj

    def arrived(copies):
        for cp, dj in copies:
            if dj is None:
                cp.wait_recv()
            else:
                @pl.when(have[-dj])
                def _():
                    cp.wait_recv()

    x_halo = [remote(x_ref.at[0, pl.ds(0, EXT)], xb.at[pl.ds(EXT + ROWS, EXT)], -1),
              remote(x_ref.at[0, pl.ds(ROWS - EXT, EXT)], xb.at[pl.ds(0, EXT)], 1)]

    u_ref = {4: (u4, EXT), 5: (u5, EXT), 6: (u6, EXT), 7: (u7, EXT), 8: (u8, 256), 9: (u9, 512), 10: (u10, 1024),
             11: (u11, 0), 12: (u12, 0), 13: (u13, 0)}

    def rows_of(ref, base, tile, shift):
        parts = [ref[pl.ds(base + r + shift, n), :] for r, n in tile]
        return parts[0] if len(parts) == 1 else jnp.concatenate(parts, axis=0)

    def state(k):
        if k < 4:
            return ((ha, hb), (hb, ha))[k % 2]
        return ha, ha

    def pre_act(k, tile, taps=None):
        d = 2 ** k
        if taps is not None:
            left, right = taps
            ref, base = u_ref[k]
            cur = rows_of(ref, base, tile, 0)
        elif k < 4:
            src = state(k)[0]
            left, cur, right = [rows_of(src, PAD, tile, o).astype(jnp.bfloat16) for o in (-d, 0, d)]
        else:
            ref, base = u_ref[k]
            left, cur, right = [rows_of(ref, base, tile, o) for o in (-d, 0, d)]
        return jnp.dot(jnp.concatenate([left, cur, right], axis=1), win[k], preferred_element_type=jnp.float32)

    def finish(k, tile, z):
        gate = jnp.tanh(z[:, :CH]) * jax.nn.sigmoid(z[:, CH:])
        pieces, off = [], 0
        for r, n in tile:
            g = gate[off:off + n]
            before, after = max(0, -r), max(0, r + n - ROWS)
            if before:
                g = jnp.concatenate([jnp.where(has_l, g[:before], 0.0), g[before:]], axis=0)
            if after:
                g = jnp.concatenate([g[:n - after], jnp.where(has_r, g[n - after:], 0.0)], axis=0)
            pieces.append(g)
            off += n
        gate = (pieces[0] if len(pieces) == 1 else jnp.concatenate(pieces, axis=0)).astype(jnp.bfloat16)
        y = jnp.dot(gate, wrs[k], preferred_element_type=jnp.float32)
        src, dst = state(k)
        off = 0
        for r, n in tile:
            new = src[pl.ds(PAD + r, n), :] + y[off:off + n, :CH]
            dst[pl.ds(PAD + r, n), :] = new
            if 4 <= k + 1 <= 13:
                ref, base = u_ref[k + 1]
                ref[pl.ds(base + r, n), :] = new.astype(jnp.bfloat16)
            lo, hi = max(r, 0), min(r + n, ROWS)
            part = y[off + lo - r:off + hi - r, CH:]
            if k == 0:
                sk[pl.ds(lo, hi - lo), :] = part
            else:
                sk[pl.ds(lo, hi - lo), :] += part
            off += n

    def run(k, tiles):
        z = {i: pre_act(k, tiles[i]) for i in range(min(2, len(tiles)))}
        for i in range(len(tiles)):
            if i + 2 < len(tiles):
                z[i + 2] = pre_act(k, tiles[i + 2])
            finish(k, tiles[i], z.pop(i))

    def weights(k):
        for c in loads[k]:
            c.wait()

    own_x.wait()
    arrived(x_halo)
    ha[pl.ds(16, ROWS + 2 * EXT), :] = xb[...].astype(jnp.float32)

    for k in range(7):
        weights(k)
        e = REACH[k]
        run(k, [[(-e, 256 + e)], [(256, 512)], [(768, 512)], [(1280, 512)], [(1792, 256 + e)]])
    weights(7)
    run(7, [[(0, 256), (1792, 256)]])
    c8 = [remote(u8.at[pl.ds(256, 256)], u8.at[pl.ds(256 + ROWS, 256)], -1),
          remote(u8.at[pl.ds(ROWS, 256)], u8.at[pl.ds(0, 256)], 1)]
    run(7, [[(256, 512)], [(768, 512)], [(1280, 512)]])

    def edge9(r):
        return remote(u9.at[pl.ds(512 + r, 256)], u9.at[pl.ds(512 + r + (ROWS if r < 512 else -ROWS), 256)], -1 if r < 512 else 1)

    weights(8)
    run(8, [[(256, 512)], [(768, 512)], [(1280, 512)]])
    c9a = [edge9(256), edge9(1536)]
    arrived(c8)
    run(8, [[(0, 256), (1792, 256)]])
    c9b = [edge9(0), edge9(1792)]

    def edge10(r, n):
        return remote(u10.at[pl.ds(1024 + r, n)], u10.at[pl.ds(1024 + r + (ROWS if r < 1024 else -ROWS), n)], -1 if r < 1024 else 1)

    weights(9)
    run(9, [[(512, 512)], [(1024, 512)]])
    c10a = [edge10(512, 512), edge10(1024, 512)]
    arrived(c9a)
    run(9, [[(0, 256), (1792, 256)]])
    c10b = [edge10(0, 256), edge10(1792, 256)]
    arrived(c9b)
    run(9, [[(256, 256), (1536, 256)]])
    c10c = [edge10(256, 256), edge10(1536, 256)]

    weights(10)
    c11 = {}

    def send11(chunks):
        for c in chunks:
            rows = pl.ds(c * CHUNK, CHUNK)
            c11[c] = [remote(u11.at[rows], v11r.at[rows], -1), remote(u11.at[rows], v11l.at[rows], 1)]

    arrived(c10a)
    run(10, [[(0, 512)], [(1536, 512)]])
    send11([0, 1, 6, 7])
    arrived(c10b)
    run(10, [[(768, 512)]])
    send11([3, 4])
    arrived(c10c)
    run(10, [[(512, 256), (1280, 256)]])
    send11([2, 5])

    weights(11)
    c12 = {}
    for c in ORDER:
        rows = pl.ds(c * CHUNK, CHUNK)
        arrived(c11[c])
        taps = jnp.where(has_l, v11l[rows, :], 0), jnp.where(has_r, v11r[rows, :], 0)
        tile = [(c * CHUNK, CHUNK)]
        finish(11, tile, pre_act(11, tile, taps))
        c12[c] = [remote(u12.at[rows], v12r.at[rows], -2), remote(u12.at[rows], v12l.at[rows], 2)]

    weights(12)
    c13 = {}
    for c in ORDER:
        rows = pl.ds(c * CHUNK, CHUNK)
        arrived(c12[c])
        taps = jnp.where(has_l2, v12l[rows, :], 0), jnp.where(has_r2, v12r[rows, :], 0)
        tile = [(c * CHUNK, CHUNK)]
        finish(12, tile, pre_act(12, tile, taps))
        c13[c] = [remote(u13.at[rows], v13.at[rows], None)]

    weights(13)
    out = []
    for c in ORDER:
        rows = pl.ds(c * CHUNK, CHUNK)
        arrived(c13[c])
        other = v13[rows, :]
        taps = jnp.where(low, 0, other), jnp.where(low, other, 0)
        tile = [(c * CHUNK, CHUNK)]
        finish(13, tile, pre_act(13, tile, taps))
        for j, cp in enumerate([pltpu.make_async_copy(ha.at[pl.ds(PAD + c * CHUNK, CHUNK)], h_ref.at[0, rows], osem.at[c, 0]),
                                pltpu.make_async_copy(sk.at[rows], s_ref.at[0, rows], osem.at[c, 1])]):
            cp.start()
            out.append(cp)

    for cp, dj in sent:
        if dj is None:
            cp.wait_send()
        else:
            @pl.when(have[dj])
            def _():
                cp.wait_send()
    for cp in out:
        cp.wait()


N_REMOTE = 2 + 2 + 4 + 6 + 16 + 16 + 8


def solution(mesh):
    act_spec = P('dp', 'sp', None)
    bf, f32 = jnp.bfloat16, jnp.float32

    def local_stack(x, w_in, w_res, w_skip):
        any_spec = pl.BlockSpec(memory_space=pl.ANY)
        u_big = [pltpu.VMEM((ROWS + 2 * EXT, CH), bf)] * 4
        return pl.pallas_call(
            kernel,
            out_shape=(jax.ShapeDtypeStruct(x.shape, f32), jax.ShapeDtypeStruct(x.shape, f32)),
            in_specs=[any_spec] * 4,
            out_specs=(any_spec, any_spec),
            scratch_shapes=[
                pltpu.VMEM((ROWS + 2 * EXT, CH), bf),
                pltpu.VMEM((ROWS + 2 * PAD, CH), f32), pltpu.VMEM((ROWS + 2 * PAD, CH), f32), pltpu.VMEM((ROWS, CH), f32),
                *u_big,
                pltpu.VMEM((ROWS + 512, CH), bf), pltpu.VMEM((ROWS + 1024, CH), bf), pltpu.VMEM((ROWS + 2048, CH), bf),
                *[pltpu.VMEM((ROWS, CH), bf)] * 8,
                pltpu.VMEM((14, 3 * CH, 2 * CH), bf), pltpu.VMEM((14, CH, 2 * CH), bf),
                pltpu.SemaphoreType.DMA, pltpu.SemaphoreType.DMA((14, 3)), pltpu.SemaphoreType.DMA((8, 2)),
                pltpu.SemaphoreType.DMA((N_REMOTE,)), pltpu.SemaphoreType.DMA((N_REMOTE,)),
            ],
            compiler_params=pltpu.CompilerParams(collective_id=0, has_side_effects=True, vmem_limit_bytes=56 * 1024 * 1024),
        )(x, w_in.reshape(14, 3 * CH, 2 * CH), w_res, w_skip)

    return jax.shard_map(local_stack, mesh=mesh, in_specs=(act_spec, P(), P(), P()), out_specs=(act_spec, act_spec), check_vma=False)
```

```python
import functools

import jax
import jax.numpy as jnp
from jax import lax
from jax.experimental import pallas as pl
from jax.experimental.pallas import tpu as pltpu
from jax.sharding import PartitionSpec as P

MESH = pl.DeviceIdType.MESH
N_DEV = 8
ROWS = 2048
CH = 128
EXT = 256
PAD = EXT + 16
REACH = [256, 256, 256, 240, 224, 192, 128, 0]
CHUNK = 256
BARRIER_AFTER = 4
ORDER = [0, 1, 6, 7, 3, 4, 2, 5]


def kernel(x_ref, win_ref, wres_ref, wskip_ref, h_ref, s_ref,
           xb, h0, h1, h2, h3, ha, sk, u4, u5, u6, u7, u8, u9, u10, u11, u12, u13,
           v11l, v11r, v12l, v12r, v13, win, wrs, lsem, wsem, osem, ssem, rsem):
    me = lax.axis_index('sp')
    has_l, has_r = me >= 1, me <= N_DEV - 2
    has_l2, has_r2 = me >= 2, me <= N_DEV - 3
    low = me < N_DEV // 2
    partner = jnp.where(low, me + N_DEV // 2, me - N_DEV // 2)
    have = {-1: has_l, 1: has_r, -2: has_l2, 2: has_r2}

    loads = []
    own_x = pltpu.make_async_copy(x_ref.at[0], xb.at[pl.ds(EXT, ROWS)], lsem)
    own_x.start()
    for k in range(14):
        trio = [pltpu.make_async_copy(win_ref.at[k], win.at[k], wsem.at[k, 0]),
                pltpu.make_async_copy(wres_ref.at[k], wrs.at[k, :, pl.ds(0, CH)], wsem.at[k, 1]),
                pltpu.make_async_copy(wskip_ref.at[k], wrs.at[k, :, pl.ds(CH, CH)], wsem.at[k, 2])]
        for c in trio:
            c.start()
        loads.append(trio)

    barrier = pltpu.get_barrier_semaphore()
    for dj, ok in have.items():
        @pl.when(ok)
        def _():
            pl.semaphore_signal(barrier, inc=1, device_id={'sp': me + dj}, device_id_type=MESH)
    pl.semaphore_signal(barrier, inc=1, device_id={'sp': partner}, device_id_type=MESH)

    def zero(ref, start, count):
        ref[pl.ds(start, count), :] = jnp.zeros((count, CH), ref.dtype)

    @pl.when(jnp.logical_not(has_l))
    def _():
        zero(xb, 0, EXT)
        zero(u8, 0, 256)
        zero(u9, 0, 512)
        zero(u10, 0, 1024)

    @pl.when(jnp.logical_not(has_r))
    def _():
        zero(xb, EXT + ROWS, EXT)
        zero(u8, 256 + ROWS, 256)
        zero(u9, 512 + ROWS, 512)
        zero(u10, 1024 + ROWS, 1024)


    count = [0]
    sent = []

    def remote(src, dst, dj):
        i = count[0]
        count[0] += 1
        dev = partner if dj is None else me + dj
        cp = pltpu.make_async_remote_copy(src_ref=src, dst_ref=dst, send_sem=ssem.at[i], recv_sem=rsem.at[i],
                                          device_id={'sp': dev}, device_id_type=MESH)
        if dj is None:
            cp.start()
        else:
            @pl.when(have[dj])
            def _():
                cp.start()
        sent.append((cp, dj))
        return cp, dj

    def arrived(copies):
        for cp, dj in copies:
            if dj is None:
                cp.wait_recv()
            else:
                @pl.when(have[-dj])
                def _():
                    cp.wait_recv()

    u_ref = {4: (u4, EXT), 5: (u5, EXT), 6: (u6, EXT), 7: (u7, EXT), 8: (u8, 256), 9: (u9, 512), 10: (u10, 1024),
             11: (u11, 0), 12: (u12, 0), 13: (u13, 0)}

    def rows_of(ref, base, tile, shift):
        parts = [ref[pl.ds(base + r + shift, n), :] for r, n in tile]
        return parts[0] if len(parts) == 1 else jnp.concatenate(parts, axis=0)

    def state(k):
        return (h0, h1, h2, h3, ha)[min(k, 4)], (h0, h1, h2, h3, ha)[min(k + 1, 4)]

    def pre_act(k, tile, taps=None):
        d = 2 ** k
        if taps is not None:
            left, right = taps
            ref, base = u_ref[k]
            cur = rows_of(ref, base, tile, 0)
        elif k < 4:
            src = state(k)[0]
            left, cur, right = [rows_of(src, PAD, tile, o).astype(jnp.bfloat16) for o in (-d, 0, d)]
        else:
            ref, base = u_ref[k]
            left, cur, right = [rows_of(ref, base, tile, o) for o in (-d, 0, d)]
        return jnp.dot(jnp.concatenate([left, cur, right], axis=1), win[k], preferred_element_type=jnp.float32)

    def finish(k, tile, z):
        gate = jnp.tanh(z[:, :CH]) * jax.nn.sigmoid(z[:, CH:])
        pieces, off = [], 0
        for r, n in tile:
            g = gate[off:off + n]
            before, after = max(0, -r), max(0, r + n - ROWS)
            if before:
                g = jnp.concatenate([jnp.where(has_l, g[:before], 0.0), g[before:]], axis=0)
            if after:
                g = jnp.concatenate([g[:n - after], jnp.where(has_r, g[n - after:], 0.0)], axis=0)
            pieces.append(g)
            off += n
        gate = (pieces[0] if len(pieces) == 1 else jnp.concatenate(pieces, axis=0)).astype(jnp.bfloat16)
        y = jnp.dot(gate, wrs[k], preferred_element_type=jnp.float32)
        src, dst = state(k)
        off = 0
        for r, n in tile:
            new = src[pl.ds(PAD + r, n), :] + y[off:off + n, :CH]
            dst[pl.ds(PAD + r, n), :] = new
            if 4 <= k + 1 <= 13:
                ref, base = u_ref[k + 1]
                ref[pl.ds(base + r, n), :] = new.astype(jnp.bfloat16)
            lo, hi = max(r, 0), min(r + n, ROWS)
            part = y[off + lo - r:off + hi - r, CH:]
            if k == 0:
                sk[pl.ds(lo, hi - lo), :] = part
            else:
                sk[pl.ds(lo, hi - lo), :] += part
            off += n

    def run(k, tiles):
        z = {i: pre_act(k, tiles[i]) for i in range(min(2, len(tiles)))}
        for i in range(len(tiles)):
            if i + 2 < len(tiles):
                z[i + 2] = pre_act(k, tiles[i + 2])
            finish(k, tiles[i], z.pop(i))

    def weights(k):
        for c in loads[k]:
            c.wait()

    own_x.wait()
    h0[pl.ds(PAD, ROWS), :] = xb[pl.ds(EXT, ROWS), :].astype(jnp.float32)
    inner = [[(i * 512, 512)] for i in range(4)]
    for k in range(BARRIER_AFTER):
        weights(k)
        run(k, inner)
    peers = 1
    for ok in have.values():
        peers += jnp.where(ok, 1, 0)
    pl.semaphore_wait(barrier, peers)
    x_halo = [remote(x_ref.at[0, pl.ds(0, EXT)], xb.at[pl.ds(EXT + ROWS, EXT)], -1),
              remote(x_ref.at[0, pl.ds(ROWS - EXT, EXT)], xb.at[pl.ds(0, EXT)], 1)]

    for k in range(BARRIER_AFTER, 7):
        weights(k)
        run(k, inner)

    arrived(x_halo)
    h0[pl.ds(16, EXT), :] = xb[pl.ds(0, EXT), :].astype(jnp.float32)
    h0[pl.ds(PAD + ROWS, EXT), :] = xb[pl.ds(EXT + ROWS, EXT), :].astype(jnp.float32)
    for k in range(7):
        e = REACH[k]
        run(k, [[(-e, 128 + e)], [(ROWS - 128, 128 + e)]])
    weights(7)
    run(7, [[(0, 256), (1792, 256)]])
    c8 = [remote(u8.at[pl.ds(256, 256)], u8.at[pl.ds(256 + ROWS, 256)], -1),
          remote(u8.at[pl.ds(ROWS, 256)], u8.at[pl.ds(0, 256)], 1)]
    run(7, [[(256, 512)], [(768, 512)], [(1280, 512)]])

    def edge9(r):
        return remote(u9.at[pl.ds(512 + r, 256)], u9.at[pl.ds(512 + r + (ROWS if r < 512 else -ROWS), 256)], -1 if r < 512 else 1)

    weights(8)
    run(8, [[(256, 512)], [(768, 512)], [(1280, 512)]])
    c9a = [edge9(256), edge9(1536)]
    arrived(c8)
    run(8, [[(0, 256), (1792, 256)]])
    c9b = [edge9(0), edge9(1792)]

    def edge10(r, n):
        return remote(u10.at[pl.ds(1024 + r, n)], u10.at[pl.ds(1024 + r + (ROWS if r < 1024 else -ROWS), n)], -1 if r < 1024 else 1)

    weights(9)
    run(9, [[(512, 512)], [(1024, 512)]])
    c10a = [edge10(512, 512), edge10(1024, 512)]
    arrived(c9a)
    run(9, [[(0, 256), (1792, 256)]])
    c10b = [edge10(0, 256), edge10(1792, 256)]
    arrived(c9b)
    run(9, [[(256, 256), (1536, 256)]])
    c10c = [edge10(256, 256), edge10(1536, 256)]

    weights(10)
    c11 = {}

    def send11(chunks):
        for c in chunks:
            rows = pl.ds(c * CHUNK, CHUNK)
            c11[c] = [remote(u11.at[rows], v11r.at[rows], -1), remote(u11.at[rows], v11l.at[rows], 1)]

    arrived(c10a)
    run(10, [[(0, 512)], [(1536, 512)]])
    send11([0, 1, 6, 7])
    arrived(c10b)
    run(10, [[(768, 512)]])
    send11([3, 4])
    arrived(c10c)
    run(10, [[(512, 256), (1280, 256)]])
    send11([2, 5])

    weights(11)
    c12 = {}
    for c in ORDER:
        rows = pl.ds(c * CHUNK, CHUNK)
        arrived(c11[c])
        taps = jnp.where(has_l, v11l[rows, :], 0), jnp.where(has_r, v11r[rows, :], 0)
        tile = [(c * CHUNK, CHUNK)]
        finish(11, tile, pre_act(11, tile, taps))
        c12[c] = [remote(u12.at[rows], v12r.at[rows], -2), remote(u12.at[rows], v12l.at[rows], 2)]

    weights(12)
    c13 = {}
    for c in ORDER:
        rows = pl.ds(c * CHUNK, CHUNK)
        arrived(c12[c])
        taps = jnp.where(has_l2, v12l[rows, :], 0), jnp.where(has_r2, v12r[rows, :], 0)
        tile = [(c * CHUNK, CHUNK)]
        finish(12, tile, pre_act(12, tile, taps))
        c13[c] = [remote(u13.at[rows], v13.at[rows], None)]

    weights(13)
    out = []
    for c in ORDER:
        rows = pl.ds(c * CHUNK, CHUNK)
        arrived(c13[c])
        other = v13[rows, :]
        taps = jnp.where(low, 0, other), jnp.where(low, other, 0)
        tile = [(c * CHUNK, CHUNK)]
        finish(13, tile, pre_act(13, tile, taps))
        for j, cp in enumerate([pltpu.make_async_copy(ha.at[pl.ds(PAD + c * CHUNK, CHUNK)], h_ref.at[0, rows], osem.at[c, 0]),
                                pltpu.make_async_copy(sk.at[rows], s_ref.at[0, rows], osem.at[c, 1])]):
            cp.start()
            out.append(cp)

    for cp, dj in sent:
        if dj is None:
            cp.wait_send()
        else:
            @pl.when(have[dj])
            def _():
                cp.wait_send()
    for cp in out:
        cp.wait()


N_REMOTE = 2 + 2 + 4 + 6 + 16 + 16 + 8


def solution(mesh):
    act_spec = P('dp', 'sp', None)
    bf, f32 = jnp.bfloat16, jnp.float32

    def local_stack(x, w_in, w_res, w_skip):
        any_spec = pl.BlockSpec(memory_space=pl.ANY)
        u_big = [pltpu.VMEM((ROWS + 2 * EXT, CH), bf)] * 4
        return pl.pallas_call(
            kernel,
            out_shape=(jax.ShapeDtypeStruct(x.shape, f32), jax.ShapeDtypeStruct(x.shape, f32)),
            in_specs=[any_spec] * 4,
            out_specs=(any_spec, any_spec),
            scratch_shapes=[
                pltpu.VMEM((ROWS + 2 * EXT, CH), bf),
                *[pltpu.VMEM((ROWS + 2 * PAD, CH), f32)] * 5, pltpu.VMEM((ROWS, CH), f32),
                *u_big,
                pltpu.VMEM((ROWS + 512, CH), bf), pltpu.VMEM((ROWS + 1024, CH), bf), pltpu.VMEM((ROWS + 2048, CH), bf),
                *[pltpu.VMEM((ROWS, CH), bf)] * 8,
                pltpu.VMEM((14, 3 * CH, 2 * CH), bf), pltpu.VMEM((14, CH, 2 * CH), bf),
                pltpu.SemaphoreType.DMA, pltpu.SemaphoreType.DMA((14, 3)), pltpu.SemaphoreType.DMA((8, 2)),
                pltpu.SemaphoreType.DMA((N_REMOTE,)), pltpu.SemaphoreType.DMA((N_REMOTE,)),
            ],
            compiler_params=pltpu.CompilerParams(collective_id=0, has_side_effects=True, vmem_limit_bytes=56 * 1024 * 1024),
        )(x, w_in.reshape(14, 3 * CH, 2 * CH), w_res, w_skip)

    return jax.shard_map(local_stack, mesh=mesh, in_specs=(act_spec, P(), P(), P()), out_specs=(act_spec, act_spec), check_vma=False)
```

```python
import functools

import jax
import jax.numpy as jnp
from jax import lax
from jax.experimental import pallas as pl
from jax.experimental.pallas import tpu as pltpu
from jax.sharding import PartitionSpec as P

MESH = pl.DeviceIdType.MESH
N_DEV = 8
ROWS = 2048
CH = 128
EXT = 256
PAD = EXT + 16
REACH = [256, 256, 256, 240, 224, 192, 128, 0]
CHUNK = 256
BARRIER_AFTER = 2
ORDER = [1, 6, 0, 7, 3, 4, 2, 5]


def kernel(x_ref, win_ref, wres_ref, wskip_ref, h_ref, s_ref,
           xb, h0, h1, h2, h3, ha, sk, u4, u5, u6, u7, u8, u9, u10, u11, u12, u13,
           v11, v12l, v12r, v13, win, wrs, lsem, wsem, osem, ssem, rsem, s11, r11):
    me = lax.axis_index('sp')
    has_l, has_r = me >= 1, me <= N_DEV - 2
    has_l2, has_r2 = me >= 2, me <= N_DEV - 3
    low = me < N_DEV // 2
    partner = jnp.where(low, me + N_DEV // 2, me - N_DEV // 2)
    even = lax.rem(me, 2) == 0
    has_o = (me >= 1) & (me <= N_DEV - 2)
    inner, outer = jnp.where(even, me + 1, me - 1), jnp.where(even, me - 1, me + 1)
    have = {-1: has_l, 1: has_r, -2: has_l2, 2: has_r2, 'outer': has_o, 'inner': None, 'partner': None}
    device = {-2: me - 2, 2: me + 2, 'outer': outer, 'inner': inner, 'partner': partner}
    across = {'inner': jnp.where(even, -ROWS, ROWS), 'outer': jnp.where(even, ROWS, -ROWS)}

    def from_inner(p, n):
        return pl.multiple_of(jnp.where(even, ROWS - p - n, p), 256)

    loads = []
    own_x = pltpu.make_async_copy(x_ref.at[0], xb.at[pl.ds(EXT, ROWS)], lsem)
    own_x.start()
    for k in range(14):
        trio = [pltpu.make_async_copy(win_ref.at[k], win.at[k], wsem.at[k, 0]),
                pltpu.make_async_copy(wres_ref.at[k], wrs.at[k, :, pl.ds(0, CH)], wsem.at[k, 1]),
                pltpu.make_async_copy(wskip_ref.at[k], wrs.at[k, :, pl.ds(CH, CH)], wsem.at[k, 2])]
        for c in trio:
            c.start()
        loads.append(trio)

    barrier = pltpu.get_barrier_semaphore()
    for dj in (-2, -1, 1, 2):
        @pl.when(have[dj])
        def _():
            pl.semaphore_signal(barrier, inc=1, device_id={'sp': me + dj}, device_id_type=MESH)
    pl.semaphore_signal(barrier, inc=1, device_id={'sp': partner}, device_id_type=MESH)

    def zero(ref, start, count):
        ref[pl.ds(start, count), :] = jnp.zeros((count, CH), ref.dtype)

    @pl.when(jnp.logical_not(has_l))
    def _():
        zero(xb, 0, EXT)
        zero(u8, 0, 256)
        zero(u9, 0, 512)
        zero(u10, 0, 1024)

    @pl.when(jnp.logical_not(has_r))
    def _():
        zero(xb, EXT + ROWS, EXT)
        zero(u8, 256 + ROWS, 256)
        zero(u9, 512 + ROWS, 512)
        zero(u10, 1024 + ROWS, 1024)


    count = [0]
    sent = []

    def start(cp, to):
        if have[to] is None:
            cp.start()
        else:
            @pl.when(have[to])
            def _():
                cp.start()

    def remote(src, dst, to):
        i = count[0]
        count[0] += 1
        cp = pltpu.make_async_remote_copy(src_ref=src, dst_ref=dst, send_sem=ssem.at[i], recv_sem=rsem.at[i],
                                          device_id={'sp': device[to]}, device_id_type=MESH)
        start(cp, to)
        sent.append((cp, to))
        return cp, to

    def arrived(copies):
        for cp, to in copies:
            came = have[-to] if isinstance(to, int) else have[to]
            if came is None:
                cp.wait_recv()
            else:
                @pl.when(came)
                def _():
                    cp.wait_recv()

    def halo(ref, base, to, p, n):
        row = base + from_inner(p, n)
        return remote(ref.at[pl.ds(row, n)], ref.at[pl.ds(row + across[to], n)], to)

    u_ref = {4: (u4, EXT), 5: (u5, EXT), 6: (u6, EXT), 7: (u7, EXT), 8: (u8, 256), 9: (u9, 512), 10: (u10, 1024),
             11: (u11, 0), 12: (u12, 0), 13: (u13, 0)}

    def rows_of(ref, base, tile, shift):
        parts = [ref[pl.ds(base + r + shift, n), :] for r, n in tile]
        return parts[0] if len(parts) == 1 else jnp.concatenate(parts, axis=0)

    def state(k):
        return (h0, h1, h2, h3, ha)[min(k, 4)], (h0, h1, h2, h3, ha)[min(k + 1, 4)]

    def pre_act(k, tile, taps=None):
        d = 2 ** k
        if taps is not None:
            left, right = taps
            ref, base = u_ref[k]
            cur = rows_of(ref, base, tile, 0)
        elif k < 4:
            src = state(k)[0]
            left, cur, right = [rows_of(src, PAD, tile, o).astype(jnp.bfloat16) for o in (-d, 0, d)]
        else:
            ref, base = u_ref[k]
            left, cur, right = [rows_of(ref, base, tile, o) for o in (-d, 0, d)]
        return jnp.dot(jnp.concatenate([left, cur, right], axis=1), win[k], preferred_element_type=jnp.float32)

    def finish(k, tile, z):
        gate = jnp.tanh(z[:, :CH]) * jax.nn.sigmoid(z[:, CH:])
        pieces, off = [], 0
        for r, n in tile:
            g = gate[off:off + n]
            before, after = (max(0, -r), max(0, r + n - ROWS)) if isinstance(r, int) else (0, 0)
            if before:
                g = jnp.concatenate([jnp.where(has_l, g[:before], 0.0), g[before:]], axis=0)
            if after:
                g = jnp.concatenate([g[:n - after], jnp.where(has_r, g[n - after:], 0.0)], axis=0)
            pieces.append(g)
            off += n
        gate = (pieces[0] if len(pieces) == 1 else jnp.concatenate(pieces, axis=0)).astype(jnp.bfloat16)
        y = jnp.dot(gate, wrs[k], preferred_element_type=jnp.float32)
        src, dst = state(k)
        off = 0
        for r, n in tile:
            new = src[pl.ds(PAD + r, n), :] + y[off:off + n, :CH]
            dst[pl.ds(PAD + r, n), :] = new
            if 4 <= k + 1 <= 13:
                ref, base = u_ref[k + 1]
                ref[pl.ds(base + r, n), :] = new.astype(jnp.bfloat16)
            lo, m = r + before, n - before - after
            part = y[off + before:off + before + m, CH:]
            if k == 0:
                sk[pl.ds(lo, m), :] = part
            else:
                sk[pl.ds(lo, m), :] += part
            off += n

    def run(k, tiles):
        z = {i: pre_act(k, tiles[i]) for i in range(min(2, len(tiles)))}
        for i in range(len(tiles)):
            if i + 2 < len(tiles):
                z[i + 2] = pre_act(k, tiles[i + 2])
            finish(k, tiles[i], z.pop(i))

    def weights(k):
        for c in loads[k]:
            c.wait()

    own_x.wait()
    h0[pl.ds(PAD, ROWS), :] = xb[pl.ds(EXT, ROWS), :].astype(jnp.float32)
    inner = [[(i * 512, 512)] for i in range(4)]
    for k in range(BARRIER_AFTER):
        weights(k)
        run(k, inner)
    peers = 1
    for dj in (-2, -1, 1, 2):
        peers += jnp.where(have[dj], 1, 0)
    pl.semaphore_wait(barrier, peers)
    x_halo = [halo(xb, EXT, 'outer', ROWS - EXT, EXT), halo(xb, EXT, 'inner', 0, EXT)]
    for k in range(BARRIER_AFTER, 7):
        weights(k)
        run(k, inner)

    arrived(x_halo)
    h0[pl.ds(16, EXT), :] = xb[pl.ds(0, EXT), :].astype(jnp.float32)
    h0[pl.ds(PAD + ROWS, EXT), :] = xb[pl.ds(EXT + ROWS, EXT), :].astype(jnp.float32)
    for k in range(7):
        e = REACH[k]
        run(k, [[(-e, 128 + e)], [(ROWS - 128, 128 + e)]])
    def side(p, n):
        return [(from_inner(p, n), n)]

    weights(7)
    run(7, [[(0, 256), (1792, 256)]])
    o8 = halo(u8, 256, 'outer', 1792, 256)
    i8 = halo(u8, 256, 'inner', 0, 256)
    run(7, [[(256, 512)], [(768, 512)], [(1280, 512)]])

    weights(8)
    arrived([i8])
    run(8, [side(0, 256), [(256, 512)], [(768, 512)], [(1280, 512)]])
    o9a = halo(u9, 512, 'outer', 1536, 256)
    i9 = halo(u9, 512, 'inner', 0, 512)
    arrived([o8])
    run(8, [side(1792, 256)])
    o9b = halo(u9, 512, 'outer', 1792, 256)

    weights(9)
    run(9, [[(512, 512)], [(1024, 512)]])
    o10a = halo(u10, 1024, 'outer', 1024, 512)
    i10a = halo(u10, 1024, 'inner', 512, 512)
    arrived([i9])
    run(9, [side(0, 512)])
    i10b = halo(u10, 1024, 'inner', 0, 512)
    arrived([o9a])
    run(9, [side(1792, 256)])
    o10b = halo(u10, 1024, 'outer', 1792, 256)
    arrived([o9b])
    run(9, [side(1536, 256)])
    o10c = halo(u10, 1024, 'outer', 1536, 256)

    weights(10)

    def copies11(c, rows):
        made = []
        for lane, to in enumerate(('outer', 'inner')):
            slot = jnp.where(even, 1 - lane, lane)
            made.append((pltpu.make_async_remote_copy(
                src_ref=u11.at[rows], dst_ref=v11.at[slot, rows], send_sem=s11.at[c, lane], recv_sem=r11.at[c, lane],
                device_id={'sp': device[to]}, device_id_type=MESH), to))
        return made

    def send11(p, n):
        for q in range(p, p + n, CHUNK):
            row = from_inner(q, CHUNK)
            for cp, to in copies11(row // CHUNK, pl.ds(row, CHUNK)):
                start(cp, to)

    arrived([i10a])
    run(10, [side(0, 512)])
    send11(0, 512)
    arrived([i10b])
    run(10, [side(512, 512)])
    send11(512, 512)
    arrived([o10a])
    run(10, [side(1536, 512)])
    send11(1536, 512)
    arrived([o10b])
    run(10, [side(1024, 256)])
    send11(1024, 256)
    arrived([o10c])
    run(10, [side(1280, 256)])
    send11(1280, 256)

    weights(11)
    c11 = {}
    c12 = {}
    for c in ORDER:
        rows = pl.ds(c * CHUNK, CHUNK)
        c11[c] = copies11(c, rows)
        arrived(c11[c])
        taps = jnp.where(has_l, v11[0, rows, :], 0), jnp.where(has_r, v11[1, rows, :], 0)
        tile = [(c * CHUNK, CHUNK)]
        finish(11, tile, pre_act(11, tile, taps))
        c12[c] = [remote(u12.at[rows], v12r.at[rows], -2), remote(u12.at[rows], v12l.at[rows], 2)]

    weights(12)
    c13 = {}
    for c in ORDER:
        rows = pl.ds(c * CHUNK, CHUNK)
        arrived(c12[c])
        taps = jnp.where(has_l2, v12l[rows, :], 0), jnp.where(has_r2, v12r[rows, :], 0)
        tile = [(c * CHUNK, CHUNK)]
        finish(12, tile, pre_act(12, tile, taps))
        c13[c] = [remote(u13.at[rows], v13.at[rows], 'partner')]

    weights(13)
    out = []
    for c in ORDER:
        rows = pl.ds(c * CHUNK, CHUNK)
        arrived(c13[c])
        other = v13[rows, :]
        taps = jnp.where(low, 0, other), jnp.where(low, other, 0)
        tile = [(c * CHUNK, CHUNK)]
        finish(13, tile, pre_act(13, tile, taps))
        for j, cp in enumerate([pltpu.make_async_copy(ha.at[pl.ds(PAD + c * CHUNK, CHUNK)], h_ref.at[0, rows], osem.at[c, 0]),
                                pltpu.make_async_copy(sk.at[rows], s_ref.at[0, rows], osem.at[c, 1])]):
            cp.start()
            out.append(cp)

    for cp, to in sent + [pair for made in c11.values() for pair in made]:
        if have[to] is None:
            cp.wait_send()
        else:
            @pl.when(have[to])
            def _():
                cp.wait_send()
    for cp in out:
        cp.wait()


N_REMOTE = 2 + 2 + 3 + 5 + 16 + 8


def solution(mesh):
    act_spec = P('dp', 'sp', None)
    bf, f32 = jnp.bfloat16, jnp.float32

    def local_stack(x, w_in, w_res, w_skip):
        any_spec = pl.BlockSpec(memory_space=pl.ANY)
        u_big = [pltpu.VMEM((ROWS + 2 * EXT, CH), bf)] * 4
        return pl.pallas_call(
            kernel,
            out_shape=(jax.ShapeDtypeStruct(x.shape, f32), jax.ShapeDtypeStruct(x.shape, f32)),
            in_specs=[any_spec] * 4,
            out_specs=(any_spec, any_spec),
            scratch_shapes=[
                pltpu.VMEM((ROWS + 2 * EXT, CH), bf),
                *[pltpu.VMEM((ROWS + 2 * PAD, CH), f32)] * 5, pltpu.VMEM((ROWS, CH), f32),
                *u_big,
                pltpu.VMEM((ROWS + 512, CH), bf), pltpu.VMEM((ROWS + 1024, CH), bf), pltpu.VMEM((ROWS + 2048, CH), bf),
                *[pltpu.VMEM((ROWS, CH), bf)] * 3, pltpu.VMEM((2, ROWS, CH), bf), *[pltpu.VMEM((ROWS, CH), bf)] * 3,
                pltpu.VMEM((14, 3 * CH, 2 * CH), bf), pltpu.VMEM((14, CH, 2 * CH), bf),
                pltpu.SemaphoreType.DMA, pltpu.SemaphoreType.DMA((14, 3)), pltpu.SemaphoreType.DMA((8, 2)),
                pltpu.SemaphoreType.DMA((N_REMOTE,)), pltpu.SemaphoreType.DMA((N_REMOTE,)),
                pltpu.SemaphoreType.DMA((8, 2)), pltpu.SemaphoreType.DMA((8, 2)),
            ],
            compiler_params=pltpu.CompilerParams(collective_id=0, has_side_effects=True, vmem_limit_bytes=56 * 1024 * 1024),
        )(x, w_in.reshape(14, 3 * CH, 2 * CH), w_res, w_skip)

    return jax.shard_map(local_stack, mesh=mesh, in_specs=(act_spec, P(), P(), P()), out_specs=(act_spec, act_spec), check_vma=False)
```

```python
import functools

import jax
import jax.numpy as jnp
from jax import lax
from jax.experimental import pallas as pl
from jax.experimental.pallas import tpu as pltpu
from jax.sharding import PartitionSpec as P

MESH = pl.DeviceIdType.MESH
N_DEV = 8
ROWS = 2048
CH = 128
EXT = 256
PAD = EXT + 16
REACH = [256, 256, 256, 240, 224, 192, 128, 0]
CHUNK = 256
BAND = [496, 512, 512, 496, 480, 448, 384, 256]
ORDER = [1, 6, 0, 7, 3, 4, 2, 5]


def kernel(x_ref, win_ref, wres_ref, wskip_ref, h_ref, s_ref,
           xb, h0, h1, h2, h3, ha, sk, u4, u5, u6, u7, u8, u9, u10, u11, u12, u13,
           v11, v12l, v12r, v13, win, wrs, lsem, wsem, osem, ssem, rsem, s11, r11):
    me = lax.axis_index('sp')
    has_l, has_r = me >= 1, me <= N_DEV - 2
    has_l2, has_r2 = me >= 2, me <= N_DEV - 3
    low = me < N_DEV // 2
    partner = jnp.where(low, me + N_DEV // 2, me - N_DEV // 2)
    even = lax.rem(me, 2) == 0
    has_o = (me >= 1) & (me <= N_DEV - 2)
    inner, outer = jnp.where(even, me + 1, me - 1), jnp.where(even, me - 1, me + 1)
    have = {-1: has_l, 1: has_r, -2: has_l2, 2: has_r2, 'outer': has_o, 'inner': None, 'partner': None}
    device = {-2: me - 2, 2: me + 2, 'outer': outer, 'inner': inner, 'partner': partner}
    across = {'inner': jnp.where(even, -ROWS, ROWS), 'outer': jnp.where(even, ROWS, -ROWS)}

    def from_inner(p, n):
        return pl.multiple_of(jnp.where(even, ROWS - p - n, p), 256)

    loads = []
    own_x = pltpu.make_async_copy(x_ref.at[0], xb.at[pl.ds(EXT, ROWS)], lsem)
    own_x.start()
    for k in range(14):
        trio = [pltpu.make_async_copy(win_ref.at[k], win.at[k], wsem.at[k, 0]),
                pltpu.make_async_copy(wres_ref.at[k], wrs.at[k, :, pl.ds(0, CH)], wsem.at[k, 1]),
                pltpu.make_async_copy(wskip_ref.at[k], wrs.at[k, :, pl.ds(CH, CH)], wsem.at[k, 2])]
        for c in trio:
            c.start()
        loads.append(trio)

    barrier = pltpu.get_barrier_semaphore()
    for dj in (-2, -1, 1, 2):
        @pl.when(have[dj])
        def _():
            pl.semaphore_signal(barrier, inc=1, device_id={'sp': me + dj}, device_id_type=MESH)
    pl.semaphore_signal(barrier, inc=1, device_id={'sp': partner}, device_id_type=MESH)

    def zero(ref, start, count):
        ref[pl.ds(start, count), :] = jnp.zeros((count, CH), ref.dtype)

    @pl.when(jnp.logical_not(has_l))
    def _():
        zero(xb, 0, EXT)
        zero(u8, 0, 256)
        zero(u9, 0, 512)
        zero(u10, 0, 1024)

    @pl.when(jnp.logical_not(has_r))
    def _():
        zero(xb, EXT + ROWS, EXT)
        zero(u8, 256 + ROWS, 256)
        zero(u9, 512 + ROWS, 512)
        zero(u10, 1024 + ROWS, 1024)


    count = [0]
    sent = []

    def start(cp, to):
        if have[to] is None:
            cp.start()
        else:
            @pl.when(have[to])
            def _():
                cp.start()

    def remote(src, dst, to):
        i = count[0]
        count[0] += 1
        cp = pltpu.make_async_remote_copy(src_ref=src, dst_ref=dst, send_sem=ssem.at[i], recv_sem=rsem.at[i],
                                          device_id={'sp': device[to]}, device_id_type=MESH)
        start(cp, to)
        sent.append((cp, to))
        return cp, to

    def arrived(copies):
        for cp, to in copies:
            came = have[-to] if isinstance(to, int) else have[to]
            if came is None:
                cp.wait_recv()
            else:
                @pl.when(came)
                def _():
                    cp.wait_recv()

    def halo(ref, base, to, p, n, source=None):
        row = from_inner(p, n)
        src = ref.at[pl.ds(base + row, n)] if source is None else source.at[0, pl.ds(row, n)]
        return remote(src, ref.at[pl.ds(base + row + across[to], n)], to)

    peers = 1
    for dj in (-2, -1, 1, 2):
        peers += jnp.where(have[dj], 1, 0)
    pl.semaphore_wait(barrier, peers)
    x_halo = [halo(xb, EXT, 'outer', ROWS - EXT, EXT, x_ref), halo(xb, EXT, 'inner', 0, EXT, x_ref)]

    u_ref = {4: (u4, EXT), 5: (u5, EXT), 6: (u6, EXT), 7: (u7, EXT), 8: (u8, 256), 9: (u9, 512), 10: (u10, 1024),
             11: (u11, 0), 12: (u12, 0), 13: (u13, 0)}

    def rows_of(ref, base, tile, shift):
        parts = [ref[pl.ds(base + r + shift, n), :] for r, n in tile]
        return parts[0] if len(parts) == 1 else jnp.concatenate(parts, axis=0)

    def state(k):
        return (h0, h1, h2, h3, ha)[min(k, 4)], (h0, h1, h2, h3, ha)[min(k + 1, 4)]

    def pre_act(k, tile, taps=None):
        d = 2 ** k
        if taps is not None:
            left, right = taps
            ref, base = u_ref[k]
            cur = rows_of(ref, base, tile, 0)
        elif k < 4:
            src = state(k)[0]
            left, cur, right = [rows_of(src, PAD, tile, o).astype(jnp.bfloat16) for o in (-d, 0, d)]
        else:
            ref, base = u_ref[k]
            left, cur, right = [rows_of(ref, base, tile, o) for o in (-d, 0, d)]
        return jnp.dot(jnp.concatenate([left, cur, right], axis=1), win[k], preferred_element_type=jnp.float32)

    def finish(k, tile, z):
        gate = jnp.tanh(z[:, :CH]) * jax.nn.sigmoid(z[:, CH:])
        pieces, off = [], 0
        for r, n in tile:
            g = gate[off:off + n]
            before, after = (max(0, -r), max(0, r + n - ROWS)) if isinstance(r, int) else (0, 0)
            if before:
                g = jnp.concatenate([jnp.where(has_l, g[:before], 0.0), g[before:]], axis=0)
            if after:
                g = jnp.concatenate([g[:n - after], jnp.where(has_r, g[n - after:], 0.0)], axis=0)
            pieces.append(g)
            off += n
        gate = (pieces[0] if len(pieces) == 1 else jnp.concatenate(pieces, axis=0)).astype(jnp.bfloat16)
        y = jnp.dot(gate, wrs[k], preferred_element_type=jnp.float32)
        src, dst = state(k)
        off = 0
        for r, n in tile:
            new = src[pl.ds(PAD + r, n), :] + y[off:off + n, :CH]
            dst[pl.ds(PAD + r, n), :] = new
            if 4 <= k + 1 <= 13:
                ref, base = u_ref[k + 1]
                ref[pl.ds(base + r, n), :] = new.astype(jnp.bfloat16)
            lo, m = r + before, n - before - after
            part = y[off + before:off + before + m, CH:]
            if k == 0:
                sk[pl.ds(lo, m), :] = part
            else:
                sk[pl.ds(lo, m), :] += part
            off += n

    waited = set()

    def weights(k):
        if k not in waited:
            waited.add(k)
            for c in loads[k]:
                c.wait()

    def reads(task, earlier):
        (k, tile), (k0, tile0) = task, earlier
        if k0 != k - 1:
            return False
        d = 2 ** k
        for r, n in tile:
            for r0, n0 in tile0:
                if not isinstance(r, int) or not isinstance(r0, int):
                    return True
                if any(r + o < r0 + n0 and r0 < r + o + n for o in (-d, 0, d)):
                    return True
        return False

    def run(tasks):
        pending = []

        def retire(count):
            for _ in range(count):
                k, tile, z = pending.pop(0)
                finish(k, tile, z)
        for task in tasks:
            weights(task[0])
            needed = [i for i, p in enumerate(pending) if reads(task, p[:2])]
            if needed:
                retire(needed[-1] + 1)
            z = pre_act(*task)
            if len(pending) == 2:
                retire(1)
            pending.append((*task, z))
        retire(len(pending))

    def split(lo, hi, count):
        cuts = [lo + (hi - lo) * i // count // 16 * 16 for i in range(count)] + [hi]
        return [[(p, q - p)] for p, q in zip(cuts, cuts[1:])]

    def interior(k):
        return [(k, t) for t in split(BAND[k], ROWS - BAND[k], 4 if k == 7 else 3 if k == 6 else 2)]

    def bands(k):
        e, b = REACH[k], BAND[k]
        n = 2 if k < 7 else 1
        return [(k, t) for t in split(-e, b, n) + split(ROWS - b, ROWS + e, n)]

    own_x.wait()
    h0[pl.ds(PAD, ROWS), :] = xb[pl.ds(EXT, ROWS), :].astype(jnp.float32)
    run(interior(0) + interior(1))
    arrived(x_halo)
    h0[pl.ds(16, EXT), :] = xb[pl.ds(0, EXT), :].astype(jnp.float32)
    h0[pl.ds(PAD + ROWS, EXT), :] = xb[pl.ds(EXT + ROWS, EXT), :].astype(jnp.float32)
    run([task for k in range(8) for task in bands(k)])

    def side(p, n):
        return [(from_inner(p, n), n)]

    o8 = halo(u8, 256, 'outer', 1792, 256)
    i8 = halo(u8, 256, 'inner', 0, 256)
    run([task for k in range(2, 8) for task in interior(k)])

    arrived([i8, o8])
    run([(8, side(1536, 512)), (8, side(0, 512))])
    o9a = halo(u9, 512, 'outer', 1536, 256)
    o9b = halo(u9, 512, 'outer', 1792, 256)
    i9 = halo(u9, 512, 'inner', 0, 512)
    run([(8, [(512, 512)]), (8, [(1024, 512)]), (9, [(512, 512)]), (9, [(1024, 512)])])
    o10a = halo(u10, 1024, 'outer', 1024, 512)
    i10a = halo(u10, 1024, 'inner', 512, 512)
    arrived([i9])
    run([(9, side(0, 512))])
    i10b = halo(u10, 1024, 'inner', 0, 512)
    arrived([o9a])
    run([(9, side(1792, 256))])
    o10b = halo(u10, 1024, 'outer', 1792, 256)
    arrived([o9b])
    run([(9, side(1536, 256))])
    o10c = halo(u10, 1024, 'outer', 1536, 256)

    weights(10)

    def copies11(c, rows):
        made = []
        for lane, to in enumerate(('outer', 'inner')):
            slot = jnp.where(even, 1 - lane, lane)
            made.append((pltpu.make_async_remote_copy(
                src_ref=u11.at[rows], dst_ref=v11.at[slot, rows], send_sem=s11.at[c, lane], recv_sem=r11.at[c, lane],
                device_id={'sp': device[to]}, device_id_type=MESH), to))
        return made

    def send11(p, n):
        for q in range(p, p + n, CHUNK):
            row = from_inner(q, CHUNK)
            for cp, to in copies11(row // CHUNK, pl.ds(row, CHUNK)):
                start(cp, to)

    arrived([i10a])
    run([(10, side(0, 512))])
    send11(0, 512)
    arrived([i10b])
    run([(10, side(512, 512))])
    send11(512, 512)
    arrived([o10a])
    run([(10, side(1536, 512))])
    send11(1536, 512)
    arrived([o10b])
    run([(10, side(1024, 256))])
    send11(1024, 256)
    arrived([o10c])
    run([(10, side(1280, 256))])
    send11(1280, 256)

    weights(11)
    c11 = {}
    c12 = {}
    for c in ORDER:
        rows = pl.ds(c * CHUNK, CHUNK)
        c11[c] = copies11(c, rows)
        arrived(c11[c])
        taps = jnp.where(has_l, v11[0, rows, :], 0), jnp.where(has_r, v11[1, rows, :], 0)
        tile = [(c * CHUNK, CHUNK)]
        finish(11, tile, pre_act(11, tile, taps))
        c12[c] = [remote(u12.at[rows], v12r.at[rows], -2), remote(u12.at[rows], v12l.at[rows], 2)]

    weights(12)
    c13 = {}
    for c in ORDER:
        rows = pl.ds(c * CHUNK, CHUNK)
        arrived(c12[c])
        taps = jnp.where(has_l2, v12l[rows, :], 0), jnp.where(has_r2, v12r[rows, :], 0)
        tile = [(c * CHUNK, CHUNK)]
        finish(12, tile, pre_act(12, tile, taps))
        c13[c] = [remote(u13.at[rows], v13.at[rows], 'partner')]

    weights(13)
    out = []
    for c in ORDER:
        rows = pl.ds(c * CHUNK, CHUNK)
        arrived(c13[c])
        other = v13[rows, :]
        taps = jnp.where(low, 0, other), jnp.where(low, other, 0)
        tile = [(c * CHUNK, CHUNK)]
        finish(13, tile, pre_act(13, tile, taps))
        for j, cp in enumerate([pltpu.make_async_copy(ha.at[pl.ds(PAD + c * CHUNK, CHUNK)], h_ref.at[0, rows], osem.at[c, 0]),
                                pltpu.make_async_copy(sk.at[rows], s_ref.at[0, rows], osem.at[c, 1])]):
            cp.start()
            out.append(cp)

    for cp, to in sent + [pair for made in c11.values() for pair in made]:
        if have[to] is None:
            cp.wait_send()
        else:
            @pl.when(have[to])
            def _():
                cp.wait_send()
    for cp in out:
        cp.wait()


N_REMOTE = 2 + 2 + 3 + 5 + 16 + 8


def solution(mesh):
    act_spec = P('dp', 'sp', None)
    bf, f32 = jnp.bfloat16, jnp.float32

    def local_stack(x, w_in, w_res, w_skip):
        any_spec = pl.BlockSpec(memory_space=pl.ANY)
        u_big = [pltpu.VMEM((ROWS + 2 * EXT, CH), bf)] * 4
        return pl.pallas_call(
            kernel,
            out_shape=(jax.ShapeDtypeStruct(x.shape, f32), jax.ShapeDtypeStruct(x.shape, f32)),
            in_specs=[any_spec] * 4,
            out_specs=(any_spec, any_spec),
            scratch_shapes=[
                pltpu.VMEM((ROWS + 2 * EXT, CH), bf),
                *[pltpu.VMEM((ROWS + 2 * PAD, CH), f32)] * 5, pltpu.VMEM((ROWS, CH), f32),
                *u_big,
                pltpu.VMEM((ROWS + 512, CH), bf), pltpu.VMEM((ROWS + 1024, CH), bf), pltpu.VMEM((ROWS + 2048, CH), bf),
                *[pltpu.VMEM((ROWS, CH), bf)] * 3, pltpu.VMEM((2, ROWS, CH), bf), *[pltpu.VMEM((ROWS, CH), bf)] * 3,
                pltpu.VMEM((14, 3 * CH, 2 * CH), bf), pltpu.VMEM((14, CH, 2 * CH), bf),
                pltpu.SemaphoreType.DMA, pltpu.SemaphoreType.DMA((14, 3)), pltpu.SemaphoreType.DMA((8, 2)),
                pltpu.SemaphoreType.DMA((N_REMOTE,)), pltpu.SemaphoreType.DMA((N_REMOTE,)),
                pltpu.SemaphoreType.DMA((8, 2)), pltpu.SemaphoreType.DMA((8, 2)),
            ],
            compiler_params=pltpu.CompilerParams(collective_id=0, has_side_effects=True, vmem_limit_bytes=56 * 1024 * 1024),
        )(x, w_in.reshape(14, 3 * CH, 2 * CH), w_res, w_skip)

    return jax.shard_map(local_stack, mesh=mesh, in_specs=(act_spec, P(), P(), P()), out_specs=(act_spec, act_spec), check_vma=False)
```

```python
import functools

import jax
import jax.numpy as jnp
from jax import lax
from jax.experimental import pallas as pl
from jax.experimental.pallas import tpu as pltpu
from jax.sharding import PartitionSpec as P

MESH = pl.DeviceIdType.MESH
N_DEV = 8
ROWS = 2048
CH = 128
EXT = 256
PAD = EXT + 16
REACH = [256, 256, 256, 240, 224, 192, 128, 0]
CHUNK = 256
AHEAD = 3
BAND = [496, 512, 512, 496, 480, 448, 384, 256]
EARLY = 2
ORDER = [1, 6, 0, 7, 3, 4, 2, 5]


def kernel(x_ref, win_ref, wres_ref, wskip_ref, h_ref, s_ref, v13,
           xb, h0, h1, h2, h3, ha, sk, u4, u5, u6, u7, u8, u9, u10, u11, u12, u13,
           v11, v12l, v12r, win, wrs, lsem, wsem, osem, ssem, rsem, s11, r11):
    me = lax.axis_index('sp')
    has_l, has_r = me >= 1, me <= N_DEV - 2
    has_l2, has_r2 = me >= 2, me <= N_DEV - 3
    low = me < N_DEV // 2
    partner = jnp.where(low, me + N_DEV // 2, me - N_DEV // 2)
    even = lax.rem(me, 2) == 0
    has_o = (me >= 1) & (me <= N_DEV - 2)
    inner, outer = jnp.where(even, me + 1, me - 1), jnp.where(even, me - 1, me + 1)
    have = {-1: has_l, 1: has_r, -2: has_l2, 2: has_r2, 'outer': has_o, 'inner': None, 'partner': None}
    device = {-2: me - 2, 2: me + 2, 'outer': outer, 'inner': inner, 'partner': partner}
    across = {'inner': jnp.where(even, -ROWS, ROWS), 'outer': jnp.where(even, ROWS, -ROWS)}

    def from_inner(p, n):
        return pl.multiple_of(jnp.where(even, ROWS - p - n, p), 256)

    loads = []
    own_x = pltpu.make_async_copy(x_ref.at[0], xb.at[pl.ds(EXT, ROWS)], lsem)
    own_x.start()
    for k in range(13):
        trio = [pltpu.make_async_copy(win_ref.at[k], win.at[k], wsem.at[k, 0]),
                pltpu.make_async_copy(wres_ref.at[k], wrs.at[k, :, pl.ds(0, CH)], wsem.at[k, 1]),
                pltpu.make_async_copy(wskip_ref.at[k], wrs.at[k, :, pl.ds(CH, CH)], wsem.at[k, 2])]
        for c in trio:
            c.start()
        loads.append(trio)

    barrier = pltpu.get_barrier_semaphore()
    for dj in (-1, 1):
        @pl.when(have[dj])
        def _():
            pl.semaphore_signal(barrier, inc=1, device_id={'sp': me + dj}, device_id_type=MESH)

    def zero(ref, start, count):
        ref[pl.ds(start, count), :] = jnp.zeros((count, CH), ref.dtype)

    @pl.when(jnp.logical_not(has_l))
    def _():
        zero(xb, 0, EXT)
        zero(u8, 0, 256)
        zero(u9, 0, 512)
        zero(u10, 0, 1024)

    @pl.when(jnp.logical_not(has_r))
    def _():
        zero(xb, EXT + ROWS, EXT)
        zero(u8, 256 + ROWS, 256)
        zero(u9, 512 + ROWS, 512)
        zero(u10, 1024 + ROWS, 1024)


    count = [0]
    sent = []

    def start(cp, to):
        if have[to] is None:
            cp.start()
        else:
            @pl.when(have[to])
            def _():
                cp.start()

    def remote(src, dst, to, now=True):
        i = count[0]
        count[0] += 1
        cp = pltpu.make_async_remote_copy(src_ref=src, dst_ref=dst, send_sem=ssem.at[i], recv_sem=rsem.at[i],
                                          device_id={'sp': device[to]}, device_id_type=MESH)
        if now:
            start(cp, to)
        sent.append((cp, to))
        return cp, to

    def arrived(copies):
        for cp, to in copies:
            came = have[-to] if isinstance(to, int) else have[to]
            if came is None:
                cp.wait_recv()
            else:
                @pl.when(came)
                def _():
                    cp.wait_recv()

    def halo(ref, base, to, p, n, source=None):
        row = from_inner(p, n)
        src = ref.at[pl.ds(base + row, n)] if source is None else source.at[0, pl.ds(row, n)]
        return remote(src, ref.at[pl.ds(base + row + across[to], n)], to)

    pl.semaphore_wait(barrier, jnp.where(has_o, 2, 1))
    x_halo = [halo(xb, EXT, 'outer', ROWS - EXT, EXT, x_ref), halo(xb, EXT, 'inner', 0, EXT, x_ref)]

    u_ref = {4: (u4, EXT), 5: (u5, EXT), 6: (u6, EXT), 7: (u7, EXT), 8: (u8, 256), 9: (u9, 512), 10: (u10, 1024),
             11: (u11, 0), 12: (u12, 0), 13: (u13, 0)}

    def rows_of(ref, base, tile, shift):
        parts = [ref[pl.ds(base + r + shift, n), :] for r, n in tile]
        return parts[0] if len(parts) == 1 else jnp.concatenate(parts, axis=0)

    def state(k):
        return (h0, h1, h2, h3, ha)[min(k, 4)], (h0, h1, h2, h3, ha)[min(k + 1, 4)]

    def pre_act(k, tile, taps=None):
        d = 2 ** k
        if taps is not None:
            left, right = taps
            ref, base = u_ref[k]
            cur = rows_of(ref, base, tile, 0)
        elif k < 4:
            src = state(k)[0]
            left, cur, right = [rows_of(src, PAD, tile, o).astype(jnp.bfloat16) for o in (-d, 0, d)]
        else:
            ref, base = u_ref[k]
            left, cur, right = [rows_of(ref, base, tile, o) for o in (-d, 0, d)]
        return jnp.dot(jnp.concatenate([left, cur, right], axis=1), win[k], preferred_element_type=jnp.float32)

    def finish(k, tile, z):
        gate = jnp.tanh(z[:, :CH]) * jax.nn.sigmoid(z[:, CH:])
        pieces, off = [], 0
        for r, n in tile:
            g = gate[off:off + n]
            before, after = (max(0, -r), max(0, r + n - ROWS)) if isinstance(r, int) else (0, 0)
            if before:
                g = jnp.concatenate([jnp.where(has_l, g[:before], 0.0), g[before:]], axis=0)
            if after:
                g = jnp.concatenate([g[:n - after], jnp.where(has_r, g[n - after:], 0.0)], axis=0)
            pieces.append(g)
            off += n
        gate = (pieces[0] if len(pieces) == 1 else jnp.concatenate(pieces, axis=0)).astype(jnp.bfloat16)
        y = jnp.dot(gate, wrs[k], preferred_element_type=jnp.float32)
        src, dst = state(k)
        off = 0
        for r, n in tile:
            new = src[pl.ds(PAD + r, n), :] + y[off:off + n, :CH]
            dst[pl.ds(PAD + r, n), :] = new
            if 4 <= k + 1 <= 13:
                ref, base = u_ref[k + 1]
                ref[pl.ds(base + r, n), :] = new.astype(jnp.bfloat16)
            lo, m = r + before, n - before - after
            part = y[off + before:off + before + m, CH:]
            if k == 0:
                sk[pl.ds(lo, m), :] = part
            else:
                sk[pl.ds(lo, m), :] += part
            off += n

    waited = set()

    def weights(k):
        if k not in waited:
            waited.add(k)
            for c in loads[k]:
                c.wait()

    def reads(task, earlier):
        (k, tile), (k0, tile0) = task, earlier
        if k0 != k - 1:
            return False
        d = 2 ** k
        for r, n in tile:
            for r0, n0 in tile0:
                if not isinstance(r, int) or not isinstance(r0, int):
                    return True
                if any(r + o < r0 + n0 and r0 < r + o + n for o in (-d, 0, d)):
                    return True
        return False

    def run(tasks):
        pending = []

        def retire(count):
            for _ in range(count):
                k, tile, z = pending.pop(0)
                finish(k, tile, z)
        for task in tasks:
            weights(task[0])
            needed = [i for i, p in enumerate(pending) if reads(task, p[:2])]
            if needed:
                retire(needed[-1] + 1)
            z = pre_act(*task)
            if len(pending) == 2:
                retire(1)
            pending.append((*task, z))
        retire(len(pending))

    def split(lo, hi, count):
        cuts = [lo + (hi - lo) * i // count // 16 * 16 for i in range(count)] + [hi]
        return [[(p, q - p)] for p, q in zip(cuts, cuts[1:])]

    def interior(k):
        return [(k, t) for t in split(BAND[k], ROWS - BAND[k], 3 if k >= 6 else 2)]

    def bands(k):
        e, b = REACH[k], BAND[k]
        n = 2 if k < 7 else 1
        return [(k, t) for t in split(-e, b, n) + split(ROWS - b, ROWS + e, n)]

    def copies11(c, rows):
        made = []
        for lane, to in enumerate(('outer', 'inner')):
            slot = jnp.where(even, 1 - lane, lane)
            made.append((pltpu.make_async_remote_copy(
                src_ref=u11.at[rows], dst_ref=v11.at[slot, rows], send_sem=s11.at[c, lane], recv_sem=r11.at[c, lane],
                device_id={'sp': device[to]}, device_id_type=MESH), to))
        return made

    def send11(p, n):
        for q in range(p, p + n, CHUNK):
            row = from_inner(q, CHUNK)
            for cp, to in copies11(row // CHUNK, pl.ds(row, CHUNK)):
                start(cp, to)

    own_x.wait()
    h0[pl.ds(PAD, ROWS), :] = xb[pl.ds(EXT, ROWS), :].astype(jnp.float32)
    run([task for k in range(EARLY) for task in interior(k)])
    arrived(x_halo)
    h0[pl.ds(16, EXT), :] = xb[pl.ds(0, EXT), :].astype(jnp.float32)
    h0[pl.ds(PAD + ROWS, EXT), :] = xb[pl.ds(EXT + ROWS, EXT), :].astype(jnp.float32)
    run([task for k in range(8) for task in bands(k)])

    def side(p, n):
        return [(from_inner(p, n), n)]

    o8 = halo(u8, 256, 'outer', 1792, 256)
    i8 = halo(u8, 256, 'inner', 0, 256)
    run([task for k in range(EARLY, 8) for task in interior(k)])

    arrived([i8, o8])
    run([(8, side(1536, 512)), (8, side(0, 512))])
    o9a = halo(u9, 512, 'outer', 1536, 256)
    o9b = halo(u9, 512, 'outer', 1792, 256)
    i9 = halo(u9, 512, 'inner', 0, 512)
    run([(8, [(512, 512)]), (8, [(1024, 512)]), (9, [(512, 512)]), (9, [(1024, 512)])])
    o10a = halo(u10, 1024, 'outer', 1024, 512)
    i10a = halo(u10, 1024, 'inner', 512, 512)
    arrived([i9])
    run([(9, side(0, 512))])
    i10b = halo(u10, 1024, 'inner', 0, 512)
    arrived([i10a])
    run([(10, side(0, 512))])
    send11(0, 512)
    arrived([o9a])
    run([(9, side(1792, 256))])
    o10b = halo(u10, 1024, 'outer', 1792, 256)
    arrived([o9b])
    run([(9, side(1536, 256))])
    o10c = halo(u10, 1024, 'outer', 1536, 256)

    arrived([i10b])
    run([(10, side(512, 512))])
    send11(512, 512)
    arrived([o10a])
    run([(10, side(1536, 512))])
    send11(1536, 512)
    arrived([o10b])
    run([(10, side(1024, 256))])
    send11(1024, 256)
    arrived([o10c])
    run([(10, side(1280, 256))])
    send11(1280, 256)

    weights(11)
    c11 = {}
    c12 = {}
    for c in ORDER:
        rows = pl.ds(c * CHUNK, CHUNK)
        c11[c] = copies11(c, rows)
        arrived(c11[c])
        taps = jnp.where(has_l, v11[0, rows, :], 0), jnp.where(has_r, v11[1, rows, :], 0)
        tile = [(c * CHUNK, CHUNK)]
        finish(11, tile, pre_act(11, tile, taps))
        c12[c] = [remote(u12.at[rows], v12r.at[rows], -2), remote(u12.at[rows], v12l.at[rows], 2)]

    weights(12)
    c13, out = {}, []
    at_end = jnp.logical_not(has_l2 & has_r2)
    for c in ORDER:
        rows = pl.ds(c * CHUNK, CHUNK)
        arrived(c12[c])
        taps = jnp.where(has_l2, v12l[rows, :], 0), jnp.where(has_r2, v12r[rows, :], 0)
        tile = [(c * CHUNK, CHUNK)]
        finish(12, tile, pre_act(12, tile, taps))
        c13[c] = [remote(u13.at[rows], v13.at[rows], 'partner', now=False)]
        if len(c13) <= AHEAD:
            start(*c13[c][0])
        else:
            @pl.when(jnp.logical_not(at_end))
            def _():
                c13[c][0][0].start()
        for j, cp in enumerate([pltpu.make_async_copy(ha.at[pl.ds(PAD + c * CHUNK, CHUNK)], h_ref.at[0, rows], osem.at[c, 0]),
                                pltpu.make_async_copy(sk.at[rows], s_ref.at[0, rows], osem.at[c, 1])]):
            cp.start()
            out.append(cp)

    for i, c in enumerate(ORDER):
        arrived(c13[c])
        if i + AHEAD < len(ORDER):
            @pl.when(at_end)
            def _():
                c13[ORDER[i + AHEAD]][0][0].start()

    for cp, to in sent + [pair for made in c11.values() for pair in made]:
        if have[to] is None:
            cp.wait_send()
        else:
            @pl.when(have[to])
            def _():
                cp.wait_send()
    for cp in out:
        cp.wait()


def last_layer(h_in, s_in, other_ref, win, wres, wskip, h_out, s_out):
    low = lax.axis_index('sp') < N_DEV // 2
    cur, other = h_in[0], other_ref[...]
    lhs = jnp.concatenate([jnp.where(low, 0, other), cur.astype(jnp.bfloat16), jnp.where(low, other, 0)], axis=1)
    z = jnp.dot(lhs, win[0], preferred_element_type=jnp.float32)
    gate = (jnp.tanh(z[:, :CH]) * jax.nn.sigmoid(z[:, CH:])).astype(jnp.bfloat16)
    y = jnp.dot(gate, jnp.concatenate([wres[0], wskip[0]], axis=1), preferred_element_type=jnp.float32)
    h_out[0] = cur + y[:, :CH]
    s_out[0] = s_in[0] + y[:, CH:]


LAST_ROWS = 1024
N_REMOTE = 2 + 2 + 3 + 5 + 16 + 8


def solution(mesh):
    act_spec = P('dp', 'sp', None)
    bf, f32 = jnp.bfloat16, jnp.float32

    def local_stack(x, w_in, w_res, w_skip):
        any_spec = pl.BlockSpec(memory_space=pl.ANY)
        u_big = [pltpu.VMEM((ROWS + 2 * EXT, CH), bf)] * 4
        wide = w_in.reshape(14, 3 * CH, 2 * CH)
        h13, s13, other = pl.pallas_call(
            kernel,
            out_shape=(jax.ShapeDtypeStruct(x.shape, f32), jax.ShapeDtypeStruct(x.shape, f32), jax.ShapeDtypeStruct((ROWS, CH), bf)),
            in_specs=[any_spec] * 4,
            out_specs=(any_spec, any_spec, any_spec),
            scratch_shapes=[
                pltpu.VMEM((ROWS + 2 * EXT, CH), bf),
                *[pltpu.VMEM((ROWS + 2 * PAD, CH), f32)] * 5, pltpu.VMEM((ROWS, CH), f32),
                *u_big,
                pltpu.VMEM((ROWS + 512, CH), bf), pltpu.VMEM((ROWS + 1024, CH), bf), pltpu.VMEM((ROWS + 2048, CH), bf),
                *[pltpu.VMEM((ROWS, CH), bf)] * 3, pltpu.VMEM((2, ROWS, CH), bf), *[pltpu.VMEM((ROWS, CH), bf)] * 2,
                pltpu.VMEM((13, 3 * CH, 2 * CH), bf), pltpu.VMEM((13, CH, 2 * CH), bf),
                pltpu.SemaphoreType.DMA, pltpu.SemaphoreType.DMA((13, 3)), pltpu.SemaphoreType.DMA((8, 2)),
                pltpu.SemaphoreType.DMA((N_REMOTE,)), pltpu.SemaphoreType.DMA((N_REMOTE,)),
                pltpu.SemaphoreType.DMA((8, 2)), pltpu.SemaphoreType.DMA((8, 2)),
            ],
            compiler_params=pltpu.CompilerParams(collective_id=0, has_side_effects=True, vmem_limit_bytes=56 * 1024 * 1024),
        )(x, wide, w_res, w_skip)
        rows = pl.BlockSpec((1, LAST_ROWS, CH), lambda i: (0, i, 0))
        return pl.pallas_call(
            last_layer,
            grid=(ROWS // LAST_ROWS,),
            out_shape=(jax.ShapeDtypeStruct(x.shape, f32), jax.ShapeDtypeStruct(x.shape, f32)),
            in_specs=[rows, rows, pl.BlockSpec((LAST_ROWS, CH), lambda i: (i, 0)),
                      pl.BlockSpec((1, 3 * CH, 2 * CH), lambda i: (13, 0, 0)),
                      pl.BlockSpec((1, CH, CH), lambda i: (13, 0, 0)), pl.BlockSpec((1, CH, CH), lambda i: (13, 0, 0))],
            out_specs=(rows, rows),
            compiler_params=pltpu.CompilerParams(vmem_limit_bytes=60 * 1024 * 1024),
        )(h13, s13, other, wide, w_res, w_skip)

    return jax.shard_map(local_stack, mesh=mesh, in_specs=(act_spec, P(), P(), P()), out_specs=(act_spec, act_spec), check_vma=False)
```

```python
import functools

import jax
import jax.numpy as jnp
from jax import lax
from jax.experimental import pallas as pl
from jax.experimental.pallas import tpu as pltpu
from jax.sharding import PartitionSpec as P

MESH = pl.DeviceIdType.MESH
N_DEV = 8
ROWS = 2048
CH = 128
EXT = 256
PAD = EXT + 16
REACH = [256, 256, 256, 240, 224, 192, 128, 0]
CHUNK = 256
AHEAD = 3
BAND = [496, 512, 512, 496, 480, 448, 384, 256]
EARLY = 2
ORDER = [1, 6, 0, 7, 3, 4, 2, 5]


def kernel(x_ref, win_ref, wres_ref, wskip_ref, h_ref, s_ref, v13,
           xb, h0, h1, h2, h3, ha, sk, u4, u5, u6, u7, u8, u9, u10, u11, u12, u13,
           v11, v12l, v12r, win, wrs, lsem, wsem, osem, ssem, rsem, s11, r11):
    me = lax.axis_index('sp')
    has_l, has_r = me >= 1, me <= N_DEV - 2
    has_l2, has_r2 = me >= 2, me <= N_DEV - 3
    low = me < N_DEV // 2
    partner = jnp.where(low, me + N_DEV // 2, me - N_DEV // 2)
    even = lax.rem(me, 2) == 0
    has_o = (me >= 1) & (me <= N_DEV - 2)
    inner, outer = jnp.where(even, me + 1, me - 1), jnp.where(even, me - 1, me + 1)
    have = {-1: has_l, 1: has_r, -2: has_l2, 2: has_r2, 'outer': has_o, 'inner': None, 'partner': None}
    device = {-2: me - 2, 2: me + 2, 'outer': outer, 'inner': inner, 'partner': partner}
    across = {'inner': jnp.where(even, -ROWS, ROWS), 'outer': jnp.where(even, ROWS, -ROWS)}

    def from_inner(p, n):
        return pl.multiple_of(jnp.where(even, ROWS - p - n, p), 256)

    loads = []
    own_x = pltpu.make_async_copy(x_ref.at[0], xb.at[pl.ds(EXT, ROWS)], lsem)
    own_x.start()
    for k in range(13):
        trio = [pltpu.make_async_copy(win_ref.at[k], win.at[k], wsem.at[k, 0]),
                pltpu.make_async_copy(wres_ref.at[k], wrs.at[k, :, pl.ds(0, CH)], wsem.at[k, 1]),
                pltpu.make_async_copy(wskip_ref.at[k], wrs.at[k, :, pl.ds(CH, CH)], wsem.at[k, 2])]
        for c in trio:
            c.start()
        loads.append(trio)

    barrier = pltpu.get_barrier_semaphore()
    for dj in (-1, 1):
        @pl.when(have[dj])
        def _():
            pl.semaphore_signal(barrier, inc=1, device_id={'sp': me + dj}, device_id_type=MESH)

    def zero(ref, start, count):
        ref[pl.ds(start, count), :] = jnp.zeros((count, CH), ref.dtype)

    @pl.when(jnp.logical_not(has_l))
    def _():
        zero(xb, 0, EXT)
        zero(u8, 0, 256)
        zero(u9, 0, 512)
        zero(u10, 0, 1024)

    @pl.when(jnp.logical_not(has_r))
    def _():
        zero(xb, EXT + ROWS, EXT)
        zero(u8, 256 + ROWS, 256)
        zero(u9, 512 + ROWS, 512)
        zero(u10, 1024 + ROWS, 1024)


    count = [0]
    sent = []

    def start(cp, to):
        if have[to] is None:
            cp.start()
        else:
            @pl.when(have[to])
            def _():
                cp.start()

    def remote(src, dst, to, now=True):
        i = count[0]
        count[0] += 1
        cp = pltpu.make_async_remote_copy(src_ref=src, dst_ref=dst, send_sem=ssem.at[i], recv_sem=rsem.at[i],
                                          device_id={'sp': device[to]}, device_id_type=MESH)
        if now:
            start(cp, to)
        sent.append((cp, to))
        return cp, to

    def arrived(copies):
        for cp, to in copies:
            came = have[-to] if isinstance(to, int) else have[to]
            if came is None:
                cp.wait_recv()
            else:
                @pl.when(came)
                def _():
                    cp.wait_recv()

    def halo(ref, base, to, p, n, source=None):
        row = from_inner(p, n)
        src = ref.at[pl.ds(base + row, n)] if source is None else source.at[0, pl.ds(row, n)]
        return remote(src, ref.at[pl.ds(base + row + across[to], n)], to)

    pl.semaphore_wait(barrier, jnp.where(has_o, 2, 1))
    x_halo = [halo(xb, EXT, 'outer', ROWS - EXT, EXT, x_ref), halo(xb, EXT, 'inner', 0, EXT, x_ref)]

    u_ref = {4: (u4, EXT), 5: (u5, EXT), 6: (u6, EXT), 7: (u7, EXT), 8: (u8, 256), 9: (u9, 512), 10: (u10, 1024),
             11: (u11, 0), 12: (u12, 0), 13: (u13, 0)}

    def rows_of(ref, base, tile, shift):
        parts = [ref[pl.ds(base + r + shift, n), :] for r, n in tile]
        return parts[0] if len(parts) == 1 else jnp.concatenate(parts, axis=0)

    def state(k):
        return (h0, h1, h2, h3, ha)[min(k, 4)], (h0, h1, h2, h3, ha)[min(k + 1, 4)]

    def pre_act(k, tile, taps=None):
        d = 2 ** k
        if taps is not None:
            left, right = taps
            ref, base = u_ref[k]
            cur = rows_of(ref, base, tile, 0)
        elif k < 4:
            src = state(k)[0]
            left, cur, right = [rows_of(src, PAD, tile, o).astype(jnp.bfloat16) for o in (-d, 0, d)]
        else:
            ref, base = u_ref[k]
            left, cur, right = [rows_of(ref, base, tile, o) for o in (-d, 0, d)]
        return jnp.dot(jnp.concatenate([left, cur, right], axis=1), win[k], preferred_element_type=jnp.float32)

    def finish(k, tile, z):
        gate = jnp.tanh(z[:, :CH]) * jax.nn.sigmoid(z[:, CH:])
        pieces, off = [], 0
        for r, n in tile:
            g = gate[off:off + n]
            before, after = (max(0, -r), max(0, r + n - ROWS)) if isinstance(r, int) else (0, 0)
            if before:
                g = jnp.concatenate([jnp.where(has_l, g[:before], 0.0), g[before:]], axis=0)
            if after:
                g = jnp.concatenate([g[:n - after], jnp.where(has_r, g[n - after:], 0.0)], axis=0)
            pieces.append(g)
            off += n
        gate = (pieces[0] if len(pieces) == 1 else jnp.concatenate(pieces, axis=0)).astype(jnp.bfloat16)
        y = jnp.dot(gate, wrs[k], preferred_element_type=jnp.float32)
        src, dst = state(k)
        off = 0
        for r, n in tile:
            new = src[pl.ds(PAD + r, n), :] + y[off:off + n, :CH]
            dst[pl.ds(PAD + r, n), :] = new
            if 4 <= k + 1 <= 13:
                ref, base = u_ref[k + 1]
                ref[pl.ds(base + r, n), :] = new.astype(jnp.bfloat16)
            lo, m = r + before, n - before - after
            part = y[off + before:off + before + m, CH:]
            if k == 0:
                sk[pl.ds(lo, m), :] = part
            else:
                sk[pl.ds(lo, m), :] += part
            off += n

    waited = set()

    def weights(k):
        if k not in waited:
            waited.add(k)
            for c in loads[k]:
                c.wait()

    def reads(task, earlier):
        (k, tile), (k0, tile0) = task, earlier
        if k0 != k - 1:
            return False
        d = 2 ** k
        for r, n in tile:
            for r0, n0 in tile0:
                if not isinstance(r, int) or not isinstance(r0, int):
                    return True
                if any(r + o < r0 + n0 and r0 < r + o + n for o in (-d, 0, d)):
                    return True
        return False

    def run(tasks):
        pending = []

        def retire(count):
            for _ in range(count):
                k, tile, z = pending.pop(0)
                finish(k, tile, z)
        for task in tasks:
            weights(task[0])
            needed = [i for i, p in enumerate(pending) if reads(task, p[:2])]
            if needed:
                retire(needed[-1] + 1)
            z = pre_act(*task)
            if len(pending) == 2:
                retire(1)
            pending.append((*task, z))
        retire(len(pending))

    def split(lo, hi, count):
        cuts = [lo + (hi - lo) * i // count // 16 * 16 for i in range(count)] + [hi]
        return [[(p, q - p)] for p, q in zip(cuts, cuts[1:])]

    def interior(k):
        return [(k, t) for t in split(BAND[k], ROWS - BAND[k], 3 if k >= 6 else 2)]

    def bands(k):
        e, b = REACH[k], BAND[k]
        n = 2 if k < 7 else 1
        return [(k, t) for t in split(-e, b, n) + split(ROWS - b, ROWS + e, n)]

    def copies11(c, rows):
        made = []
        for lane, to in enumerate(('outer', 'inner')):
            slot = jnp.where(even, 1 - lane, lane)
            made.append((pltpu.make_async_remote_copy(
                src_ref=u11.at[rows], dst_ref=v11.at[slot, rows], send_sem=s11.at[c, lane], recv_sem=r11.at[c, lane],
                device_id={'sp': device[to]}, device_id_type=MESH), to))
        return made

    def send11(p, n):
        for q in range(p, p + n, CHUNK):
            row = from_inner(q, CHUNK)
            for cp, to in copies11(row // CHUNK, pl.ds(row, CHUNK)):
                start(cp, to)

    own_x.wait()
    h0[pl.ds(PAD, ROWS), :] = xb[pl.ds(EXT, ROWS), :].astype(jnp.float32)
    run([task for k in range(EARLY) for task in interior(k)])
    arrived(x_halo)
    h0[pl.ds(16, EXT), :] = xb[pl.ds(0, EXT), :].astype(jnp.float32)
    h0[pl.ds(PAD + ROWS, EXT), :] = xb[pl.ds(EXT + ROWS, EXT), :].astype(jnp.float32)
    run([task for k in range(8) for task in bands(k)])

    def side(p, n):
        return [(from_inner(p, n), n)]

    o8 = halo(u8, 256, 'outer', 1792, 256)
    i8 = halo(u8, 256, 'inner', 0, 256)
    run([task for k in range(EARLY, 8) for task in interior(k)])

    arrived([i8, o8])
    run([(8, side(1536, 512)), (8, side(0, 512))])
    o9a = halo(u9, 512, 'outer', 1536, 256)
    o9b = halo(u9, 512, 'outer', 1792, 256)
    i9 = halo(u9, 512, 'inner', 0, 512)
    run([(8, [(512, 512)]), (8, [(1024, 512)]), (9, [(512, 512)]), (9, [(1024, 512)])])
    o10a = halo(u10, 1024, 'outer', 1024, 512)
    i10a = halo(u10, 1024, 'inner', 512, 512)
    arrived([i9])
    run([(9, side(0, 512))])
    i10b = halo(u10, 1024, 'inner', 0, 512)
    arrived([i10a])
    run([(10, side(0, 512))])
    send11(0, 512)
    arrived([o9a])
    run([(9, side(1792, 256))])
    o10b = halo(u10, 1024, 'outer', 1792, 256)
    arrived([o9b])
    run([(9, side(1536, 256))])
    o10c = halo(u10, 1024, 'outer', 1536, 256)

    arrived([i10b])
    run([(10, side(512, 512))])
    send11(512, 512)
    arrived([o10a])
    run([(10, side(1536, 512))])
    send11(1536, 512)
    arrived([o10b])
    run([(10, side(1024, 256))])
    send11(1024, 256)
    arrived([o10c])
    run([(10, side(1280, 256))])
    send11(1280, 256)

    weights(11)
    c11 = {}
    c12 = {}
    for c in ORDER:
        rows = pl.ds(c * CHUNK, CHUNK)
        c11[c] = copies11(c, rows)
        arrived(c11[c])
        taps = jnp.where(has_l, v11[0, rows, :], 0), jnp.where(has_r, v11[1, rows, :], 0)
        tile = [(c * CHUNK, CHUNK)]
        finish(11, tile, pre_act(11, tile, taps))
        c12[c] = [remote(u12.at[rows], v12r.at[rows], -2), remote(u12.at[rows], v12l.at[rows], 2)]

    weights(12)
    c13, out = {}, []
    at_end = jnp.logical_not(has_r2)
    for c in ORDER:
        rows = pl.ds(c * CHUNK, CHUNK)
        arrived(c12[c])
        taps = jnp.where(has_l2, v12l[rows, :], 0), jnp.where(has_r2, v12r[rows, :], 0)
        tile = [(c * CHUNK, CHUNK)]
        finish(12, tile, pre_act(12, tile, taps))
        c13[c] = [remote(u13.at[rows], v13.at[rows], 'partner', now=False)]
        if len(c13) <= AHEAD:
            start(*c13[c][0])
        else:
            @pl.when(jnp.logical_not(at_end))
            def _():
                c13[c][0][0].start()
        for j, cp in enumerate([pltpu.make_async_copy(ha.at[pl.ds(PAD + c * CHUNK, CHUNK)], h_ref.at[0, rows], osem.at[c, 0]),
                                pltpu.make_async_copy(sk.at[rows], s_ref.at[0, rows], osem.at[c, 1])]):
            cp.start()
            out.append(cp)

    for i, c in enumerate(ORDER):
        arrived(c13[c])
        if i + AHEAD < len(ORDER):
            @pl.when(at_end)
            def _():
                c13[ORDER[i + AHEAD]][0][0].start()

    for cp, to in sent + [pair for made in c11.values() for pair in made]:
        if have[to] is None:
            cp.wait_send()
        else:
            @pl.when(have[to])
            def _():
                cp.wait_send()
    for cp in out:
        cp.wait()


def last_layer(h_in, s_in, other_ref, win, wres, wskip, h_out, s_out):
    low = lax.axis_index('sp') < N_DEV // 2
    taps = win[0, pl.ds(pl.multiple_of(jnp.where(low, CH, 0), CH), 2 * CH), :]
    out_w = jnp.concatenate([wres[0], wskip[0]], axis=1)
    parts = [pl.ds(i * 512, 512) for i in range(LAST_ROWS // 512)]

    def pre_act(r):
        cur, other = h_in[0, r, :].astype(jnp.bfloat16), other_ref[r, :]
        lhs = jnp.concatenate([jnp.where(low, cur, other), jnp.where(low, other, cur)], axis=1)
        return jnp.dot(lhs, taps, preferred_element_type=jnp.float32)

    z = [pre_act(r) for r in parts]
    for r, zr in zip(parts, z):
        gate = (jnp.tanh(zr[:, :CH]) * jax.nn.sigmoid(zr[:, CH:])).astype(jnp.bfloat16)
        y = jnp.dot(gate, out_w, preferred_element_type=jnp.float32)
        h_out[0, r, :] = h_in[0, r, :] + y[:, :CH]
        s_out[0, r, :] = s_in[0, r, :] + y[:, CH:]


LAST_ROWS = 1024
N_REMOTE = 2 + 2 + 3 + 5 + 16 + 8


def solution(mesh):
    act_spec = P('dp', 'sp', None)
    bf, f32 = jnp.bfloat16, jnp.float32

    def local_stack(x, w_in, w_res, w_skip):
        any_spec = pl.BlockSpec(memory_space=pl.ANY)
        u_big = [pltpu.VMEM((ROWS + 2 * EXT, CH), bf)] * 4
        wide = w_in.reshape(14, 3 * CH, 2 * CH)
        h13, s13, other = pl.pallas_call(
            kernel,
            out_shape=(jax.ShapeDtypeStruct(x.shape, f32), jax.ShapeDtypeStruct(x.shape, f32), jax.ShapeDtypeStruct((ROWS, CH), bf)),
            in_specs=[any_spec] * 4,
            out_specs=(any_spec, any_spec, any_spec),
            scratch_shapes=[
                pltpu.VMEM((ROWS + 2 * EXT, CH), bf),
                *[pltpu.VMEM((ROWS + 2 * PAD, CH), f32)] * 5, pltpu.VMEM((ROWS, CH), f32),
                *u_big,
                pltpu.VMEM((ROWS + 512, CH), bf), pltpu.VMEM((ROWS + 1024, CH), bf), pltpu.VMEM((ROWS + 2048, CH), bf),
                *[pltpu.VMEM((ROWS, CH), bf)] * 3, pltpu.VMEM((2, ROWS, CH), bf), *[pltpu.VMEM((ROWS, CH), bf)] * 2,
                pltpu.VMEM((13, 3 * CH, 2 * CH), bf), pltpu.VMEM((13, CH, 2 * CH), bf),
                pltpu.SemaphoreType.DMA, pltpu.SemaphoreType.DMA((13, 3)), pltpu.SemaphoreType.DMA((8, 2)),
                pltpu.SemaphoreType.DMA((N_REMOTE,)), pltpu.SemaphoreType.DMA((N_REMOTE,)),
                pltpu.SemaphoreType.DMA((8, 2)), pltpu.SemaphoreType.DMA((8, 2)),
            ],
            compiler_params=pltpu.CompilerParams(collective_id=0, has_side_effects=True, vmem_limit_bytes=56 * 1024 * 1024),
        )(x, wide, w_res, w_skip)
        rows = pl.BlockSpec((1, LAST_ROWS, CH), lambda i: (0, i, 0))
        return pl.pallas_call(
            last_layer,
            grid=(ROWS // LAST_ROWS,),
            out_shape=(jax.ShapeDtypeStruct(x.shape, f32), jax.ShapeDtypeStruct(x.shape, f32)),
            in_specs=[rows, rows, pl.BlockSpec((LAST_ROWS, CH), lambda i: (i, 0)),
                      pl.BlockSpec((1, 3 * CH, 2 * CH), lambda i: (13, 0, 0)),
                      pl.BlockSpec((1, CH, CH), lambda i: (13, 0, 0)), pl.BlockSpec((1, CH, CH), lambda i: (13, 0, 0))],
            out_specs=(rows, rows),
            compiler_params=pltpu.CompilerParams(vmem_limit_bytes=60 * 1024 * 1024),
        )(h13, s13, other, wide, w_res, w_skip)

    return jax.shard_map(local_stack, mesh=mesh, in_specs=(act_spec, P(), P(), P()), out_specs=(act_spec, act_spec), check_vma=False)
```

```python
import functools

import jax
import jax.numpy as jnp
from jax import lax
from jax.experimental import pallas as pl
from jax.experimental.pallas import tpu as pltpu
from jax.sharding import PartitionSpec as P

MESH = pl.DeviceIdType.MESH
N_DEV = 8
ROWS = 2048
CH = 128
EXT = 256
PAD = EXT + 16
REACH = [256, 256, 256, 240, 224, 192, 128, 0]
CHUNK = 256
AHEAD = (5, 3)
BAND = [496, 512, 512, 496, 480, 448, 384, 256]
EARLY = 2
ORDER = [1, 6, 0, 7, 3, 4, 2, 5]


def kernel(x_ref, win_ref, wres_ref, wskip_ref, h_ref, s_ref, v13,
           xb, h0, h1, h2, h3, ha, sk, u4, u5, u6, u7, u8, u9, u10, u11, u12, u13,
           v11, v12l, v12r, win, wrs, lsem, wsem, osem, ssem, rsem, s11, r11):
    me = lax.axis_index('sp')
    has_l, has_r = me >= 1, me <= N_DEV - 2
    has_l2, has_r2 = me >= 2, me <= N_DEV - 3
    low = me < N_DEV // 2
    partner = jnp.where(low, me + N_DEV // 2, me - N_DEV // 2)
    even = lax.rem(me, 2) == 0
    has_o = (me >= 1) & (me <= N_DEV - 2)
    inner, outer = jnp.where(even, me + 1, me - 1), jnp.where(even, me - 1, me + 1)
    have = {-1: has_l, 1: has_r, -2: has_l2, 2: has_r2, 'outer': has_o, 'inner': None, 'partner': None}
    device = {-2: me - 2, 2: me + 2, 'outer': outer, 'inner': inner, 'partner': partner}
    across = {'inner': jnp.where(even, -ROWS, ROWS), 'outer': jnp.where(even, ROWS, -ROWS)}

    def from_inner(p, n):
        return pl.multiple_of(jnp.where(even, ROWS - p - n, p), 256)

    loads = []
    own_x = pltpu.make_async_copy(x_ref.at[0], xb.at[pl.ds(EXT, ROWS)], lsem)
    own_x.start()
    for k in range(13):
        trio = [pltpu.make_async_copy(win_ref.at[k], win.at[k], wsem.at[k, 0]),
                pltpu.make_async_copy(wres_ref.at[k], wrs.at[k, :, pl.ds(0, CH)], wsem.at[k, 1]),
                pltpu.make_async_copy(wskip_ref.at[k], wrs.at[k, :, pl.ds(CH, CH)], wsem.at[k, 2])]
        for c in trio:
            c.start()
        loads.append(trio)

    barrier = pltpu.get_barrier_semaphore()
    for dj in (-1, 1):
        @pl.when(have[dj])
        def _():
            pl.semaphore_signal(barrier, inc=1, device_id={'sp': me + dj}, device_id_type=MESH)

    def zero(ref, start, count):
        ref[pl.ds(start, count), :] = jnp.zeros((count, CH), ref.dtype)

    @pl.when(jnp.logical_not(has_l))
    def _():
        zero(xb, 0, EXT)
        zero(u8, 0, 256)
        zero(u9, 0, 512)
        zero(u10, 0, 1024)

    @pl.when(jnp.logical_not(has_r))
    def _():
        zero(xb, EXT + ROWS, EXT)
        zero(u8, 256 + ROWS, 256)
        zero(u9, 512 + ROWS, 512)
        zero(u10, 1024 + ROWS, 1024)


    count = [0]
    sent = []

    def start(cp, to):
        if have[to] is None:
            cp.start()
        else:
            @pl.when(have[to])
            def _():
                cp.start()

    def remote(src, dst, to, now=True):
        i = count[0]
        count[0] += 1
        cp = pltpu.make_async_remote_copy(src_ref=src, dst_ref=dst, send_sem=ssem.at[i], recv_sem=rsem.at[i],
                                          device_id={'sp': device[to]}, device_id_type=MESH)
        if now:
            start(cp, to)
        sent.append((cp, to))
        return cp, to

    def arrived(copies):
        for cp, to in copies:
            came = have[-to] if isinstance(to, int) else have[to]
            if came is None:
                cp.wait_recv()
            else:
                @pl.when(came)
                def _():
                    cp.wait_recv()

    def halo(ref, base, to, p, n, source=None):
        row = from_inner(p, n)
        src = ref.at[pl.ds(base + row, n)] if source is None else source.at[0, pl.ds(row, n)]
        return remote(src, ref.at[pl.ds(base + row + across[to], n)], to)

    pl.semaphore_wait(barrier, jnp.where(has_o, 2, 1))
    x_halo = [halo(xb, EXT, 'outer', ROWS - EXT, EXT, x_ref), halo(xb, EXT, 'inner', 0, EXT, x_ref)]

    u_ref = {4: (u4, EXT), 5: (u5, EXT), 6: (u6, EXT), 7: (u7, EXT), 8: (u8, 256), 9: (u9, 512), 10: (u10, 1024),
             11: (u11, 0), 12: (u12, 0), 13: (u13, 0)}

    def rows_of(ref, base, tile, shift):
        parts = [ref[pl.ds(base + r + shift, n), :] for r, n in tile]
        return parts[0] if len(parts) == 1 else jnp.concatenate(parts, axis=0)

    def state(k):
        return (h0, h1, h2, h3, ha)[min(k, 4)], (h0, h1, h2, h3, ha)[min(k + 1, 4)]

    def pre_act(k, tile, taps=None):
        d = 2 ** k
        if taps is not None:
            left, right = taps
            ref, base = u_ref[k]
            cur = rows_of(ref, base, tile, 0)
        elif k < 4:
            src = state(k)[0]
            left, cur, right = [rows_of(src, PAD, tile, o).astype(jnp.bfloat16) for o in (-d, 0, d)]
        else:
            ref, base = u_ref[k]
            left, cur, right = [rows_of(ref, base, tile, o) for o in (-d, 0, d)]
        return jnp.dot(jnp.concatenate([left, cur, right], axis=1), win[k], preferred_element_type=jnp.float32)

    def finish(k, tile, z):
        gate = jnp.tanh(z[:, :CH]) * jax.nn.sigmoid(z[:, CH:])
        pieces, off = [], 0
        for r, n in tile:
            g = gate[off:off + n]
            before, after = (max(0, -r), max(0, r + n - ROWS)) if isinstance(r, int) else (0, 0)
            if before:
                g = jnp.concatenate([jnp.where(has_l, g[:before], 0.0), g[before:]], axis=0)
            if after:
                g = jnp.concatenate([g[:n - after], jnp.where(has_r, g[n - after:], 0.0)], axis=0)
            pieces.append(g)
            off += n
        gate = (pieces[0] if len(pieces) == 1 else jnp.concatenate(pieces, axis=0)).astype(jnp.bfloat16)
        y = jnp.dot(gate, wrs[k], preferred_element_type=jnp.float32)
        src, dst = state(k)
        off = 0
        for r, n in tile:
            new = src[pl.ds(PAD + r, n), :] + y[off:off + n, :CH]
            dst[pl.ds(PAD + r, n), :] = new
            if 4 <= k + 1 <= 13:
                ref, base = u_ref[k + 1]
                ref[pl.ds(base + r, n), :] = new.astype(jnp.bfloat16)
            lo, m = r + before, n - before - after
            part = y[off + before:off + before + m, CH:]
            if k == 0:
                sk[pl.ds(lo, m), :] = part
            else:
                sk[pl.ds(lo, m), :] += part
            off += n

    waited = set()

    def weights(k):
        if k not in waited:
            waited.add(k)
            for c in loads[k]:
                c.wait()

    def reads(task, earlier):
        (k, tile), (k0, tile0) = task, earlier
        if k0 != k - 1:
            return False
        d = 2 ** k
        for r, n in tile:
            for r0, n0 in tile0:
                if not isinstance(r, int) or not isinstance(r0, int):
                    return True
                if any(r + o < r0 + n0 and r0 < r + o + n for o in (-d, 0, d)):
                    return True
        return False

    def run(tasks):
        pending = []

        def retire(count):
            for _ in range(count):
                k, tile, z = pending.pop(0)
                finish(k, tile, z)
        for task in tasks:
            weights(task[0])
            needed = [i for i, p in enumerate(pending) if reads(task, p[:2])]
            if needed:
                retire(needed[-1] + 1)
            z = pre_act(*task)
            if len(pending) == 2:
                retire(1)
            pending.append((*task, z))
        retire(len(pending))

    def split(lo, hi, count):
        cuts = [lo + (hi - lo) * i // count // 16 * 16 for i in range(count)] + [hi]
        return [[(p, q - p)] for p, q in zip(cuts, cuts[1:])]

    def interior(k):
        return [(k, t) for t in split(BAND[k], ROWS - BAND[k], 3 if k >= 6 else 2)]

    def bands(k):
        e, b = REACH[k], BAND[k]
        n = 2 if k < 7 else 1
        return [(k, t) for t in split(-e, b, n) + split(ROWS - b, ROWS + e, n)]

    def copies11(c, rows):
        made = []
        for lane, to in enumerate(('outer', 'inner')):
            slot = jnp.where(even, 1 - lane, lane)
            made.append((pltpu.make_async_remote_copy(
                src_ref=u11.at[rows], dst_ref=v11.at[slot, rows], send_sem=s11.at[c, lane], recv_sem=r11.at[c, lane],
                device_id={'sp': device[to]}, device_id_type=MESH), to))
        return made

    def send11(p, n):
        for q in range(p, p + n, CHUNK):
            row = from_inner(q, CHUNK)
            for cp, to in copies11(row // CHUNK, pl.ds(row, CHUNK)):
                start(cp, to)

    own_x.wait()
    h0[pl.ds(PAD, ROWS), :] = xb[pl.ds(EXT, ROWS), :].astype(jnp.float32)
    run([task for k in range(EARLY) for task in interior(k)])
    arrived(x_halo)
    h0[pl.ds(16, EXT), :] = xb[pl.ds(0, EXT), :].astype(jnp.float32)
    h0[pl.ds(PAD + ROWS, EXT), :] = xb[pl.ds(EXT + ROWS, EXT), :].astype(jnp.float32)
    run([task for k in range(8) for task in bands(k)])

    def side(p, n):
        return [(from_inner(p, n), n)]

    o8 = halo(u8, 256, 'outer', 1792, 256)
    i8 = halo(u8, 256, 'inner', 0, 256)
    run([task for k in range(EARLY, 8) for task in interior(k)])

    arrived([i8, o8])
    run([(8, side(1536, 512)), (8, side(0, 512))])
    o9a = halo(u9, 512, 'outer', 1536, 256)
    o9b = halo(u9, 512, 'outer', 1792, 256)
    i9 = halo(u9, 512, 'inner', 0, 512)
    run([(8, [(512, 512)]), (8, [(1024, 512)]), (9, [(512, 512)]), (9, [(1024, 512)])])
    o10a = halo(u10, 1024, 'outer', 1024, 512)
    i10a = halo(u10, 1024, 'inner', 512, 512)
    arrived([i9])
    run([(9, side(0, 512))])
    i10b = halo(u10, 1024, 'inner', 0, 512)
    arrived([i10a])
    run([(10, side(0, 512))])
    send11(0, 512)
    arrived([o9a])
    run([(9, side(1792, 256))])
    o10b = halo(u10, 1024, 'outer', 1792, 256)
    arrived([o9b])
    run([(9, side(1536, 256))])
    o10c = halo(u10, 1024, 'outer', 1536, 256)

    arrived([i10b])
    run([(10, side(512, 512))])
    send11(512, 512)
    arrived([o10a])
    run([(10, side(1536, 512))])
    send11(1536, 512)
    arrived([o10b])
    run([(10, side(1024, 256))])
    send11(1024, 256)
    arrived([o10c])
    run([(10, side(1280, 256))])
    send11(1280, 256)

    weights(11)
    c11 = {}
    c12 = {}
    for c in ORDER:
        rows = pl.ds(c * CHUNK, CHUNK)
        c11[c] = copies11(c, rows)
        arrived(c11[c])
        taps = jnp.where(has_l, v11[0, rows, :], 0), jnp.where(has_r, v11[1, rows, :], 0)
        tile = [(c * CHUNK, CHUNK)]
        finish(11, tile, pre_act(11, tile, taps))
        c12[c] = [remote(u12.at[rows], v12r.at[rows], -2), remote(u12.at[rows], v12l.at[rows], 2)]

    weights(12)
    c13, out = {}, []
    ends = (jnp.logical_not(has_l2), jnp.logical_not(has_r2))
    for c in ORDER:
        rows = pl.ds(c * CHUNK, CHUNK)
        arrived(c12[c])
        taps = jnp.where(has_l2, v12l[rows, :], 0), jnp.where(has_r2, v12r[rows, :], 0)
        tile = [(c * CHUNK, CHUNK)]
        finish(12, tile, pre_act(12, tile, taps))
        c13[c] = [remote(u13.at[rows], v13.at[rows], 'partner', now=False)]
        waits = [end for end, ahead in zip(ends, AHEAD) if len(c13) > ahead]
        if waits:
            @pl.when(jnp.logical_not(functools.reduce(jnp.logical_or, waits)))
            def _():
                c13[c][0][0].start()
        else:
            start(*c13[c][0])
        for j, cp in enumerate([pltpu.make_async_copy(ha.at[pl.ds(PAD + c * CHUNK, CHUNK)], h_ref.at[0, rows], osem.at[c, 0]),
                                pltpu.make_async_copy(sk.at[rows], s_ref.at[0, rows], osem.at[c, 1])]):
            cp.start()
            out.append(cp)

    for i, c in enumerate(ORDER):
        arrived(c13[c])
        for end, ahead in zip(ends, AHEAD):
            if i + ahead < len(ORDER):
                @pl.when(end)
                def _():
                    c13[ORDER[i + ahead]][0][0].start()

    for cp, to in sent + [pair for made in c11.values() for pair in made]:
        if have[to] is None:
            cp.wait_send()
        else:
            @pl.when(have[to])
            def _():
                cp.wait_send()
    for cp in out:
        cp.wait()


def last_layer(h_in, s_in, other_ref, win, wres, wskip, h_out, s_out):
    low = lax.axis_index('sp') < N_DEV // 2
    taps = win[0, pl.ds(pl.multiple_of(jnp.where(low, CH, 0), CH), 2 * CH), :]
    out_w = jnp.concatenate([wres[0], wskip[0]], axis=1)
    parts = [pl.ds(i * 512, 512) for i in range(LAST_ROWS // 512)]

    def pre_act(r):
        cur, other = h_in[0, r, :].astype(jnp.bfloat16), other_ref[r, :]
        lhs = jnp.concatenate([jnp.where(low, cur, other), jnp.where(low, other, cur)], axis=1)
        return jnp.dot(lhs, taps, preferred_element_type=jnp.float32)

    z = [pre_act(r) for r in parts]
    for r, zr in zip(parts, z):
        gate = (jnp.tanh(zr[:, :CH]) * jax.nn.sigmoid(zr[:, CH:])).astype(jnp.bfloat16)
        y = jnp.dot(gate, out_w, preferred_element_type=jnp.float32)
        h_out[0, r, :] = h_in[0, r, :] + y[:, :CH]
        s_out[0, r, :] = s_in[0, r, :] + y[:, CH:]


LAST_ROWS = 1024
N_REMOTE = 2 + 2 + 3 + 5 + 16 + 8


def solution(mesh):
    act_spec = P('dp', 'sp', None)
    bf, f32 = jnp.bfloat16, jnp.float32

    def local_stack(x, w_in, w_res, w_skip):
        any_spec = pl.BlockSpec(memory_space=pl.ANY)
        u_big = [pltpu.VMEM((ROWS + 2 * EXT, CH), bf)] * 4
        wide = w_in.reshape(14, 3 * CH, 2 * CH)
        h13, s13, other = pl.pallas_call(
            kernel,
            out_shape=(jax.ShapeDtypeStruct(x.shape, f32), jax.ShapeDtypeStruct(x.shape, f32), jax.ShapeDtypeStruct((ROWS, CH), bf)),
            in_specs=[any_spec] * 4,
            out_specs=(any_spec, any_spec, any_spec),
            scratch_shapes=[
                pltpu.VMEM((ROWS + 2 * EXT, CH), bf),
                *[pltpu.VMEM((ROWS + 2 * PAD, CH), f32)] * 5, pltpu.VMEM((ROWS, CH), f32),
                *u_big,
                pltpu.VMEM((ROWS + 512, CH), bf), pltpu.VMEM((ROWS + 1024, CH), bf), pltpu.VMEM((ROWS + 2048, CH), bf),
                *[pltpu.VMEM((ROWS, CH), bf)] * 3, pltpu.VMEM((2, ROWS, CH), bf), *[pltpu.VMEM((ROWS, CH), bf)] * 2,
                pltpu.VMEM((13, 3 * CH, 2 * CH), bf), pltpu.VMEM((13, CH, 2 * CH), bf),
                pltpu.SemaphoreType.DMA, pltpu.SemaphoreType.DMA((13, 3)), pltpu.SemaphoreType.DMA((8, 2)),
                pltpu.SemaphoreType.DMA((N_REMOTE,)), pltpu.SemaphoreType.DMA((N_REMOTE,)),
                pltpu.SemaphoreType.DMA((8, 2)), pltpu.SemaphoreType.DMA((8, 2)),
            ],
            compiler_params=pltpu.CompilerParams(collective_id=0, has_side_effects=True, vmem_limit_bytes=56 * 1024 * 1024),
        )(x, wide, w_res, w_skip)
        rows = pl.BlockSpec((1, LAST_ROWS, CH), lambda i: (0, i, 0))
        return pl.pallas_call(
            last_layer,
            grid=(ROWS // LAST_ROWS,),
            out_shape=(jax.ShapeDtypeStruct(x.shape, f32), jax.ShapeDtypeStruct(x.shape, f32)),
            in_specs=[rows, rows, pl.BlockSpec((LAST_ROWS, CH), lambda i: (i, 0)),
                      pl.BlockSpec((1, 3 * CH, 2 * CH), lambda i: (13, 0, 0)),
                      pl.BlockSpec((1, CH, CH), lambda i: (13, 0, 0)), pl.BlockSpec((1, CH, CH), lambda i: (13, 0, 0))],
            out_specs=(rows, rows),
            compiler_params=pltpu.CompilerParams(vmem_limit_bytes=60 * 1024 * 1024),
        )(h13, s13, other, wide, w_res, w_skip)

    return jax.shard_map(local_stack, mesh=mesh, in_specs=(act_spec, P(), P(), P()), out_specs=(act_spec, act_spec), check_vma=False)
```

```python
import functools

import jax
import jax.numpy as jnp
from jax import lax
from jax.experimental import pallas as pl
from jax.experimental.pallas import tpu as pltpu
from jax.sharding import PartitionSpec as P

MESH = pl.DeviceIdType.MESH
N_DEV = 8
ROWS = 2048
CH = 128
EXT = 256
PAD = EXT + 16
REACH = [256, 256, 256, 240, 224, 192, 128, 0]
CHUNK = 256
AHEAD = (4, 3)
BAND = [496, 512, 512, 496, 480, 448, 384, 256]
EARLY = 2
ORDER = [1, 6, 0, 7, 3, 4, 2, 5]


def kernel(x_ref, win_ref, wres_ref, wskip_ref, h_ref, s_ref, v13,
           xb, h0, h1, h2, h3, ha, sk, u4, u5, u6, u7, u8, u9, u10, u11, u12, u13,
           v11, v12l, v12r, win, wrs, lsem, wsem, osem, ssem, rsem, s11, r11):
    me = lax.axis_index('sp')
    has_l, has_r = me >= 1, me <= N_DEV - 2
    has_l2, has_r2 = me >= 2, me <= N_DEV - 3
    low = me < N_DEV // 2
    partner = jnp.where(low, me + N_DEV // 2, me - N_DEV // 2)
    even = lax.rem(me, 2) == 0
    has_o = (me >= 1) & (me <= N_DEV - 2)
    inner, outer = jnp.where(even, me + 1, me - 1), jnp.where(even, me - 1, me + 1)
    have = {-1: has_l, 1: has_r, -2: has_l2, 2: has_r2, 'outer': has_o, 'inner': None, 'partner': None}
    device = {-2: me - 2, 2: me + 2, 'outer': outer, 'inner': inner, 'partner': partner}
    across = {'inner': jnp.where(even, -ROWS, ROWS), 'outer': jnp.where(even, ROWS, -ROWS)}

    def from_inner(p, n):
        return pl.multiple_of(jnp.where(even, ROWS - p - n, p), 256)

    loads = []
    own_x = pltpu.make_async_copy(x_ref.at[0], xb.at[pl.ds(EXT, ROWS)], lsem)
    own_x.start()
    for k in range(13):
        trio = [pltpu.make_async_copy(win_ref.at[k], win.at[k], wsem.at[k, 0]),
                pltpu.make_async_copy(wres_ref.at[k], wrs.at[k, :, pl.ds(0, CH)], wsem.at[k, 1]),
                pltpu.make_async_copy(wskip_ref.at[k], wrs.at[k, :, pl.ds(CH, CH)], wsem.at[k, 2])]
        for c in trio:
            c.start()
        loads.append(trio)

    barrier = pltpu.get_barrier_semaphore()
    for dj in (-1, 1):
        @pl.when(have[dj])
        def _():
            pl.semaphore_signal(barrier, inc=1, device_id={'sp': me + dj}, device_id_type=MESH)

    def zero(ref, start, count):
        ref[pl.ds(start, count), :] = jnp.zeros((count, CH), ref.dtype)

    @pl.when(jnp.logical_not(has_l))
    def _():
        zero(xb, 0, EXT)
        zero(u8, 0, 256)
        zero(u9, 0, 512)
        zero(u10, 0, 1024)

    @pl.when(jnp.logical_not(has_r))
    def _():
        zero(xb, EXT + ROWS, EXT)
        zero(u8, 256 + ROWS, 256)
        zero(u9, 512 + ROWS, 512)
        zero(u10, 1024 + ROWS, 1024)


    count = [0]
    sent = []

    def start(cp, to):
        if have[to] is None:
            cp.start()
        else:
            @pl.when(have[to])
            def _():
                cp.start()

    def remote(src, dst, to, now=True):
        i = count[0]
        count[0] += 1
        cp = pltpu.make_async_remote_copy(src_ref=src, dst_ref=dst, send_sem=ssem.at[i], recv_sem=rsem.at[i],
                                          device_id={'sp': device[to]}, device_id_type=MESH)
        if now:
            start(cp, to)
        sent.append((cp, to))
        return cp, to

    def arrived(copies):
        for cp, to in copies:
            came = have[-to] if isinstance(to, int) else have[to]
            if came is None:
                cp.wait_recv()
            else:
                @pl.when(came)
                def _():
                    cp.wait_recv()

    def halo(ref, base, to, p, n, source=None):
        row = from_inner(p, n)
        src = ref.at[pl.ds(base + row, n)] if source is None else source.at[0, pl.ds(row, n)]
        return remote(src, ref.at[pl.ds(base + row + across[to], n)], to)

    pl.semaphore_wait(barrier, jnp.where(has_o, 2, 1))
    x_halo = [halo(xb, EXT, 'outer', ROWS - EXT, EXT, x_ref), halo(xb, EXT, 'inner', 0, EXT, x_ref)]

    u_ref = {4: (u4, EXT), 5: (u5, EXT), 6: (u6, EXT), 7: (u7, EXT), 8: (u8, 256), 9: (u9, 512), 10: (u10, 1024),
             11: (u11, 0), 12: (u12, 0), 13: (u13, 0)}

    def rows_of(ref, base, tile, shift):
        parts = [ref[pl.ds(base + r + shift, n), :] for r, n in tile]
        return parts[0] if len(parts) == 1 else jnp.concatenate(parts, axis=0)

    def state(k):
        return (h0, h1, h2, h3, ha)[min(k, 4)], (h0, h1, h2, h3, ha)[min(k + 1, 4)]

    def pre_act(k, tile, taps=None):
        d = 2 ** k
        if taps is not None:
            left, right = taps
            ref, base = u_ref[k]
            cur = rows_of(ref, base, tile, 0)
        elif k < 4:
            src = state(k)[0]
            left, cur, right = [rows_of(src, PAD, tile, o).astype(jnp.bfloat16) for o in (-d, 0, d)]
        else:
            ref, base = u_ref[k]
            left, cur, right = [rows_of(ref, base, tile, o) for o in (-d, 0, d)]
        return jnp.dot(jnp.concatenate([left, cur, right], axis=1), win[k], preferred_element_type=jnp.float32)

    def finish(k, tile, z):
        gate = jnp.tanh(z[:, :CH]) * jax.nn.sigmoid(z[:, CH:])
        pieces, off = [], 0
        for r, n in tile:
            g = gate[off:off + n]
            before, after = (max(0, -r), max(0, r + n - ROWS)) if isinstance(r, int) else (0, 0)
            if before:
                g = jnp.concatenate([jnp.where(has_l, g[:before], 0.0), g[before:]], axis=0)
            if after:
                g = jnp.concatenate([g[:n - after], jnp.where(has_r, g[n - after:], 0.0)], axis=0)
            pieces.append(g)
            off += n
        gate = (pieces[0] if len(pieces) == 1 else jnp.concatenate(pieces, axis=0)).astype(jnp.bfloat16)
        y = jnp.dot(gate, wrs[k], preferred_element_type=jnp.float32)
        src, dst = state(k)
        off = 0
        for r, n in tile:
            new = src[pl.ds(PAD + r, n), :] + y[off:off + n, :CH]
            dst[pl.ds(PAD + r, n), :] = new
            if 4 <= k + 1 <= 13:
                ref, base = u_ref[k + 1]
                ref[pl.ds(base + r, n), :] = new.astype(jnp.bfloat16)
            lo, m = r + before, n - before - after
            part = y[off + before:off + before + m, CH:]
            if k == 0:
                sk[pl.ds(lo, m), :] = part
            else:
                sk[pl.ds(lo, m), :] += part
            off += n

    waited = set()

    def weights(k):
        if k not in waited:
            waited.add(k)
            for c in loads[k]:
                c.wait()

    def reads(task, earlier):
        (k, tile), (k0, tile0) = task, earlier
        if k0 != k - 1:
            return False
        d = 2 ** k
        for r, n in tile:
            for r0, n0 in tile0:
                if not isinstance(r, int) or not isinstance(r0, int):
                    return True
                if any(r + o < r0 + n0 and r0 < r + o + n for o in (-d, 0, d)):
                    return True
        return False

    def run(tasks):
        pending = []

        def retire(count):
            for _ in range(count):
                k, tile, z = pending.pop(0)
                finish(k, tile, z)
        for task in tasks:
            weights(task[0])
            needed = [i for i, p in enumerate(pending) if reads(task, p[:2])]
            if needed:
                retire(needed[-1] + 1)
            z = pre_act(*task)
            if len(pending) == 2:
                retire(1)
            pending.append((*task, z))
        retire(len(pending))

    def split(lo, hi, count):
        cuts = [lo + (hi - lo) * i // count // 16 * 16 for i in range(count)] + [hi]
        return [[(p, q - p)] for p, q in zip(cuts, cuts[1:])]

    def interior(k):
        return [(k, t) for t in split(BAND[k], ROWS - BAND[k], 3 if k >= 6 else 2)]

    def bands(k):
        e, b = REACH[k], BAND[k]
        n = 2 if k < 7 else 1
        return [(k, t) for t in split(-e, b, n) + split(ROWS - b, ROWS + e, n)]

    def copies11(c, rows):
        made = []
        for lane, to in enumerate(('outer', 'inner')):
            slot = jnp.where(even, 1 - lane, lane)
            made.append((pltpu.make_async_remote_copy(
                src_ref=u11.at[rows], dst_ref=v11.at[slot, rows], send_sem=s11.at[c, lane], recv_sem=r11.at[c, lane],
                device_id={'sp': device[to]}, device_id_type=MESH), to))
        return made

    def send11(p, n):
        for q in range(p, p + n, CHUNK):
            row = from_inner(q, CHUNK)
            for cp, to in copies11(row // CHUNK, pl.ds(row, CHUNK)):
                start(cp, to)

    own_x.wait()
    h0[pl.ds(PAD, ROWS), :] = xb[pl.ds(EXT, ROWS), :].astype(jnp.float32)
    run([task for k in range(EARLY) for task in interior(k)])
    arrived(x_halo)
    h0[pl.ds(16, EXT), :] = xb[pl.ds(0, EXT), :].astype(jnp.float32)
    h0[pl.ds(PAD + ROWS, EXT), :] = xb[pl.ds(EXT + ROWS, EXT), :].astype(jnp.float32)
    run([task for k in range(8) for task in bands(k)])

    def side(p, n):
        return [(from_inner(p, n), n)]

    o8 = halo(u8, 256, 'outer', 1792, 256)
    i8 = halo(u8, 256, 'inner', 0, 256)
    run([task for k in range(EARLY, 8) for task in interior(k)])

    arrived([i8, o8])
    run([(8, side(1536, 512)), (8, side(0, 512))])
    o9a = halo(u9, 512, 'outer', 1536, 256)
    o9b = halo(u9, 512, 'outer', 1792, 256)
    i9 = halo(u9, 512, 'inner', 0, 512)
    run([(8, [(512, 512)]), (8, [(1024, 512)]), (9, [(512, 512)]), (9, [(1024, 512)])])
    o10a = halo(u10, 1024, 'outer', 1024, 512)
    i10a = halo(u10, 1024, 'inner', 512, 512)
    arrived([i9])
    run([(9, side(0, 512))])
    i10b = halo(u10, 1024, 'inner', 0, 512)
    arrived([i10a])
    run([(10, side(0, 512))])
    send11(0, 512)
    arrived([o9a])
    run([(9, side(1792, 256))])
    o10b = halo(u10, 1024, 'outer', 1792, 256)
    arrived([o9b])
    run([(9, side(1536, 256))])
    o10c = halo(u10, 1024, 'outer', 1536, 256)

    arrived([i10b])
    run([(10, side(512, 512))])
    send11(512, 512)
    arrived([o10a])
    run([(10, side(1536, 512))])
    send11(1536, 512)
    arrived([o10b])
    run([(10, side(1024, 256))])
    send11(1024, 256)
    arrived([o10c])
    run([(10, side(1280, 256))])
    send11(1280, 256)

    weights(11)
    c11 = {}
    c12 = {}
    for c in ORDER:
        rows = pl.ds(c * CHUNK, CHUNK)
        c11[c] = copies11(c, rows)
        arrived(c11[c])
        taps = jnp.where(has_l, v11[0, rows, :], 0), jnp.where(has_r, v11[1, rows, :], 0)
        tile = [(c * CHUNK, CHUNK)]
        finish(11, tile, pre_act(11, tile, taps))
        c12[c] = [remote(u12.at[rows], v12r.at[rows], -2), remote(u12.at[rows], v12l.at[rows], 2)]

    weights(12)
    c13, out = {}, []
    ends = (jnp.logical_not(has_l2), jnp.logical_not(has_r2))
    for c in ORDER:
        rows = pl.ds(c * CHUNK, CHUNK)
        arrived(c12[c])
        taps = jnp.where(has_l2, v12l[rows, :], 0), jnp.where(has_r2, v12r[rows, :], 0)
        tile = [(c * CHUNK, CHUNK)]
        finish(12, tile, pre_act(12, tile, taps))
        c13[c] = [remote(u13.at[rows], v13.at[rows], 'partner', now=False)]
        waits = [end for end, ahead in zip(ends, AHEAD) if len(c13) > ahead]
        if waits:
            @pl.when(jnp.logical_not(functools.reduce(jnp.logical_or, waits)))
            def _():
                c13[c][0][0].start()
        else:
            start(*c13[c][0])
        for j, cp in enumerate([pltpu.make_async_copy(ha.at[pl.ds(PAD + c * CHUNK, CHUNK)], h_ref.at[0, rows], osem.at[c, 0]),
                                pltpu.make_async_copy(sk.at[rows], s_ref.at[0, rows], osem.at[c, 1])]):
            cp.start()
            out.append(cp)

    for i, c in enumerate(ORDER):
        arrived(c13[c])
        for end, ahead in zip(ends, AHEAD):
            if i + ahead < len(ORDER):
                @pl.when(end)
                def _():
                    c13[ORDER[i + ahead]][0][0].start()

    for cp, to in sent + [pair for made in c11.values() for pair in made]:
        if have[to] is None:
            cp.wait_send()
        else:
            @pl.when(have[to])
            def _():
                cp.wait_send()
    for cp in out:
        cp.wait()


def last_layer(h_in, s_in, other_ref, win, wres, wskip, h_out, s_out):
    low = lax.axis_index('sp') < N_DEV // 2
    taps = win[0, pl.ds(pl.multiple_of(jnp.where(low, CH, 0), CH), 2 * CH), :]
    out_w = jnp.concatenate([wres[0], wskip[0]], axis=1)
    parts = [pl.ds(i * 512, 512) for i in range(LAST_ROWS // 512)]

    def pre_act(r):
        cur, other = h_in[0, r, :].astype(jnp.bfloat16), other_ref[r, :]
        lhs = jnp.concatenate([jnp.where(low, cur, other), jnp.where(low, other, cur)], axis=1)
        return jnp.dot(lhs, taps, preferred_element_type=jnp.float32)

    z = [pre_act(r) for r in parts]
    for r, zr in zip(parts, z):
        gate = (jnp.tanh(zr[:, :CH]) * jax.nn.sigmoid(zr[:, CH:])).astype(jnp.bfloat16)
        y = jnp.dot(gate, out_w, preferred_element_type=jnp.float32)
        h_out[0, r, :] = h_in[0, r, :] + y[:, :CH]
        s_out[0, r, :] = s_in[0, r, :] + y[:, CH:]


LAST_ROWS = 1024
N_REMOTE = 2 + 2 + 3 + 5 + 16 + 8


def solution(mesh):
    act_spec = P('dp', 'sp', None)
    bf, f32 = jnp.bfloat16, jnp.float32

    def local_stack(x, w_in, w_res, w_skip):
        any_spec = pl.BlockSpec(memory_space=pl.ANY)
        u_big = [pltpu.VMEM((ROWS + 2 * EXT, CH), bf)] * 4
        wide = w_in.reshape(14, 3 * CH, 2 * CH)
        h13, s13, other = pl.pallas_call(
            kernel,
            out_shape=(jax.ShapeDtypeStruct(x.shape, f32), jax.ShapeDtypeStruct(x.shape, f32), jax.ShapeDtypeStruct((ROWS, CH), bf)),
            in_specs=[any_spec] * 4,
            out_specs=(any_spec, any_spec, any_spec),
            scratch_shapes=[
                pltpu.VMEM((ROWS + 2 * EXT, CH), bf),
                *[pltpu.VMEM((ROWS + 2 * PAD, CH), f32)] * 5, pltpu.VMEM((ROWS, CH), f32),
                *u_big,
                pltpu.VMEM((ROWS + 512, CH), bf), pltpu.VMEM((ROWS + 1024, CH), bf), pltpu.VMEM((ROWS + 2048, CH), bf),
                *[pltpu.VMEM((ROWS, CH), bf)] * 3, pltpu.VMEM((2, ROWS, CH), bf), *[pltpu.VMEM((ROWS, CH), bf)] * 2,
                pltpu.VMEM((13, 3 * CH, 2 * CH), bf), pltpu.VMEM((13, CH, 2 * CH), bf),
                pltpu.SemaphoreType.DMA, pltpu.SemaphoreType.DMA((13, 3)), pltpu.SemaphoreType.DMA((8, 2)),
                pltpu.SemaphoreType.DMA((N_REMOTE,)), pltpu.SemaphoreType.DMA((N_REMOTE,)),
                pltpu.SemaphoreType.DMA((8, 2)), pltpu.SemaphoreType.DMA((8, 2)),
            ],
            compiler_params=pltpu.CompilerParams(collective_id=0, has_side_effects=True, vmem_limit_bytes=56 * 1024 * 1024),
        )(x, wide, w_res, w_skip)
        rows = pl.BlockSpec((1, LAST_ROWS, CH), lambda i: (0, i, 0))
        return pl.pallas_call(
            last_layer,
            grid=(ROWS // LAST_ROWS,),
            out_shape=(jax.ShapeDtypeStruct(x.shape, f32), jax.ShapeDtypeStruct(x.shape, f32)),
            in_specs=[rows, rows, pl.BlockSpec((LAST_ROWS, CH), lambda i: (i, 0)),
                      pl.BlockSpec((1, 3 * CH, 2 * CH), lambda i: (13, 0, 0)),
                      pl.BlockSpec((1, CH, CH), lambda i: (13, 0, 0)), pl.BlockSpec((1, CH, CH), lambda i: (13, 0, 0))],
            out_specs=(rows, rows),
            compiler_params=pltpu.CompilerParams(vmem_limit_bytes=60 * 1024 * 1024),
        )(h13, s13, other, wide, w_res, w_skip)

    return jax.shard_map(local_stack, mesh=mesh, in_specs=(act_spec, P(), P(), P()), out_specs=(act_spec, act_spec), check_vma=False)
```
